32 devices in a mesh: dp: 8 (over y, x, core), mp: 4 (over z).
Axes of the slice: x: 2, y: 2, z: 4, core: 2. Of those that a mesh axis runs over, the one named last changes fastest.
Arguments:
- hidden: bfloat16 [16384, 4096], P('dp', 'mp'), may hold values from -600 to 600
- segments: int32 [128, 128], P('dp'), may hold values from 0 to 5, never falling along the last dimension, each value on 1 to 40 neighbouring positions
- counts: int32 [8], replicated, may hold values from 1 to 16, 64 in all
- dest_order: int32 [8], replicated, may hold values from 0 to 7, each once
- norm_gain: bfloat16 [4096], replicated, may hold values from 0.5 to 1.5
- q_weight: bfloat16 [4096, 4096], P(None, 'mp'), may hold values from -1.921875 to 1.921875
- kv_weight: bfloat16 [4096, 2048], P(None, 'mp'), may hold values from -0.09375 to 0.09375
Outputs:
- attended: bfloat16 [8192, 4096], P('dp', 'mp')
The draws below stay inside these ranges and needn't reach their ends.
Inputs may be any that keep to these rules, and one draw needn't show every extreme that they name: counts sum to 64 and reach 16 on some index of dp. `segments`: ids never fall within a block; a hypothesis spans at most 40 tokens.
All inputs are finite; a program needn't handle non-finite values.
Results may differ from the reference program's by a relative error of at most 0.0073.
Values may be sent and summed in bfloat16 or wider, within the bound.
No kernel may reach another device: no remote copies, remote signals or barrier semaphores. Data moves between devices by JAX's collectives and lax.ppermute only.
A program may use at most 128 MiB of HBM per device.

```python
import math
import jax
import jax.numpy as jnp
import numpy as np
from jax import lax

D = 4096
HQ = 32
KV = 8
HD = 128
BLOCK = 128
KEEP = 8
SLOTS = 16
SHARE = 1
BLOCKS = 128
ROWS = 16384
N_DP = 8


def weight_bases(key):
    scale = D ** (-0.5)
    key_part = jnp.clip(jax.random.normal(jax.random.fold_in(key, 11), (D, KV, HD), jnp.float32), -6.0, 6.0) * scale
    value_part = jnp.clip(jax.random.normal(jax.random.fold_in(key, 12), (D, KV, HD), jnp.float32), -6.0, 6.0) * scale
    return (key_part, value_part)


def draw_hidden(key, part):
    columns = 10.0 ** (jnp.arange(D, dtype=jnp.float32) / D)
    scales = 10.0 ** jax.random.uniform(jax.random.fold_in(key, 22), (ROWS, 1), jnp.float32)
    base = jnp.clip(jax.random.normal(jax.random.fold_in(key, 21), (ROWS, D), jnp.float32), -6.0, 6.0)
    return (base * columns[None, :] * scales).astype(jnp.bfloat16)


def draw_q_weight(key, part):
    noise = jnp.clip(jax.random.normal(jax.random.fold_in(key, 13), (D, HQ, HD), jnp.float32), -6.0, 6.0) * D ** (-0.5)
    result = noise
    return result.reshape(D, HQ * HD).astype(jnp.bfloat16)


def draw_kv_weight(key, part):
    key_part, value_part = weight_bases(key)
    piece = HD // SHARE
    stacked = jnp.stack([key_part.reshape(D, KV, SHARE, piece), value_part.reshape(D, KV, SHARE, piece)], axis=3)
    return stacked.reshape(D, 2 * KV * HD).astype(jnp.bfloat16)


def split_up(count, total, most, slope):
    portions = [(1 << 20) // math.isqrt(grade ** slope) + 1 for grade in range(2, count + 1)]
    rest, given = total - most - (count - 1), [1] * (count - 1)
    while rest > 0:
        free = [i for i in range(count - 1) if given[i] < most]
        pool, budget = sum([portions[i] for i in free]), rest
        for i in free:
            more = min(most - given[i], max(1, budget * portions[i] // pool), rest)
            given[i] = given[i] + more
            rest = rest - more
    return np.array([most] + given)


def ragged(own_key, number_of, total, reach, lean):
    if number_of == 2:
        one = jax.random.randint(own_key, (), max(1, total - reach), min(reach, total - 1) + 1)
        return jnp.stack([one, total - one])
    sizes = jnp.asarray(split_up(number_of, total, reach, lean), jnp.int32)
    twos = (number_of - 1) // 2
    source_of, receiver = sizes[1:1 + 2 * twos:2], sizes[2:2 + 2 * twos:2]
    margin = jnp.minimum(source_of - 1, reach - receiver)
    moved = jax.random.randint(jax.random.fold_in(own_key, 1), (twos,), 0, 1 << 20) % (margin + 1)
    sizes = sizes.at[1:1 + 2 * twos:2].set(source_of - moved).at[2:2 + 2 * twos:2].set(receiver + moved)
    return sizes[jax.random.permutation(jax.random.fold_in(own_key, 2), number_of)]


def setup_inputs(seed: int = 0) -> dict:
    keys = jax.random.split(jax.random.key(seed), 8)
    return {
        "hidden": draw_hidden(jax.random.fold_in(keys[7], 71), 0),
        "segments": jax.vmap(lambda own: jnp.searchsorted(jnp.cumsum(ragged(own, 6, BLOCK, 40, 0)), jnp.arange(BLOCK), side="right"))(jax.random.split(keys[1], BLOCKS)).reshape((BLOCKS, BLOCK)).astype(jnp.int32),
        "counts": ragged(keys[2], N_DP, N_DP * KEEP, SLOTS, 2).astype(jnp.int32),
        "dest_order": jax.random.permutation(keys[3], N_DP).astype(jnp.int32),
        "norm_gain": jnp.clip(1.0 + 0.1 * jax.random.normal(keys[4], (D,), jnp.float32), 0.5, 1.5).astype(jnp.bfloat16),
        "q_weight": draw_q_weight(jax.random.fold_in(keys[7], 71), 0),
        "kv_weight": draw_kv_weight(jax.random.fold_in(keys[7], 71), 0),
    }


epsilon = 1e-05
rope_base = 500000.0

def rope_tables(positions, width):
    halves = width // 2
    frequency = rope_base ** (-(jnp.arange(halves, dtype=jnp.float32) * 2.0) / width)
    angles = positions.astype(jnp.float32)[..., None] * frequency
    return (jnp.cos(angles), jnp.sin(angles))

def rotate(tensor, cosine, sine_part):
    halves = tensor.shape[-1] // 2
    lower = tensor[..., :halves]
    upper = tensor[..., halves:]
    cosine = cosine[..., None, :]
    sine_part = sine_part[..., None, :]
    return jnp.concatenate([lower * cosine - upper * sine_part, upper * cosine + lower * sine_part], axis=-1)

def segment_masks(block_segments):
    length = block_segments.shape[-1]
    column = jnp.arange(length, dtype=jnp.int32)
    same_segment = block_segments[:, :, None] == block_segments[:, None, :]
    before = column[None, :] < column[:, None]
    positions = lax.optimization_barrier(jnp.sum((same_segment & before[None]).astype(jnp.int32), axis=2))
    visible = same_segment & (column[None, :] <= column[:, None])[None]
    return (positions, visible)

def attend(rows, block_segments, norm_gain, q_weight, k_weight, v_weight):
    count_blocks = block_segments.shape[0]
    block_len = block_segments.shape[1]
    widened = rows.astype(jnp.float32)
    row_scale = lax.rsqrt(lax.optimization_barrier(jnp.mean(widened * widened, axis=1, keepdims=True)) + epsilon)
    normed = (widened * norm_gain.astype(jnp.float32)).astype(jnp.bfloat16)
    queries = row_scale * jnp.dot(normed, q_weight, preferred_element_type=jnp.float32)
    key_raw = (row_scale * jnp.dot(normed, k_weight, preferred_element_type=jnp.float32)).astype(jnp.bfloat16)
    value_rows = (row_scale * jnp.dot(normed, v_weight, preferred_element_type=jnp.float32)).astype(jnp.bfloat16)
    positions, visible = segment_masks(block_segments)
    cosine, sine_part = rope_tables(positions, HD)
    query_rows = rotate(queries.reshape(count_blocks, block_len, HQ, HD), cosine, sine_part).astype(jnp.bfloat16)
    key_rows = rotate(key_raw.astype(jnp.float32).reshape(count_blocks, block_len, KV, HD), cosine, sine_part).astype(jnp.bfloat16)
    values = value_rows.reshape(count_blocks, block_len, KV, HD)
    grouped = query_rows.reshape(count_blocks, block_len, KV, HQ // KV, HD)
    scores = jnp.einsum('nikgd,njkd->nkgij', grouped.astype(jnp.float32), key_rows.astype(jnp.float32)) * HD ** (-0.5)
    scores = jnp.where(visible[:, None, None], scores, -jnp.inf)
    highest = lax.optimization_barrier(jnp.max(scores, axis=-1, keepdims=True))
    weights = jnp.exp(scores - highest)
    shares = (weights / lax.optimization_barrier(jnp.sum(weights, axis=-1, keepdims=True))).astype(jnp.bfloat16)
    mixture = jnp.einsum('nkgij,njkd->nikgd', shares.astype(jnp.float32), values.astype(jnp.float32))
    return mixture.reshape(count_blocks * block_len, HQ * HD).astype(jnp.bfloat16)

def reference(hidden, segments, counts, dest_order, norm_gain, q_weight, kv_weight):
    device_ids = jnp.arange(N_DP, dtype=jnp.int32)
    starts = (jnp.cumsum(counts) - counts).astype(jnp.int32)
    finishes = (starts + counts).astype(jnp.int32)
    position_of = lax.optimization_barrier(jnp.sum(device_ids[None, :] * (dest_order[None, :] == device_ids[:, None]).astype(jnp.int32), axis=1)).astype(jnp.int32)
    global_ids = (jnp.arange(KEEP, dtype=jnp.int32)[None, :] * N_DP + position_of[:, None]).astype(jnp.int32)
    sources = lax.optimization_barrier(jnp.sum((finishes[None, None, :] <= global_ids[:, :, None]).astype(jnp.int32), axis=2)).astype(jnp.int32)
    picked = (sources * SLOTS + global_ids - starts[sources]).reshape(-1).astype(jnp.int32)
    blocks = hidden.reshape(BLOCKS, BLOCK, D)[picked].reshape(N_DP, KEEP * BLOCK, D)
    block_segments = segments[picked].reshape(N_DP, KEEP, BLOCK)
    kv_split = kv_weight.reshape(D, KV, SHARE, 2, HD // SHARE)
    k_weight = kv_split[:, :, :, 0, :].reshape(D, KV * HD)
    v_weight = kv_split[:, :, :, 1, :].reshape(D, KV * HD)

    def one_device(inputs):
        return attend(inputs[0], inputs[1], norm_gain, q_weight, k_weight, v_weight)
    outputs = lax.map(one_device, (blocks, block_segments))
    return outputs.reshape(N_DP * KEEP * BLOCK, HQ * HD)
```

```python
import functools

import jax
import jax.numpy as jnp
from jax import lax
from jax.experimental import pallas as pl
from jax.experimental.pallas import tpu as pltpu
from jax.sharding import PartitionSpec as P

KV = 8
HD = 128


epsilon = 1e-05
rope_base = 500000.0

ID_ROWS = 8
FEATURE_EIGHTHS = (2, 6)
GROUPS = (2, 2, 2, 2)


def for_sending(array):
    return jax.tree.map(lambda a: a.astype(jnp.bfloat16) if a.dtype == jnp.float32 else a, array)


def swapped(value, axis, stride):
    mask = 2**stride
    pairs = [(source, source ^ mask) for source in range(lax.axis_size(axis))]
    return lax.ppermute(value, axis, pairs)


def rope_tables(positions, width):
    halves = width // 2
    frequency = rope_base ** (-(jnp.arange(halves, dtype=jnp.float32) * 2.0) / width)
    angles = positions.astype(jnp.float32)[..., None] * frequency
    return (jnp.cos(angles), jnp.sin(angles))


def rotate(tensor, cosine, sine_part):
    halves = tensor.shape[-1] // 2
    lower = tensor[..., :halves]
    upper = tensor[..., halves:]
    cosine = cosine[..., None, :]
    sine_part = sine_part[..., None, :]
    return jnp.concatenate(
        [lower * cosine - upper * sine_part, upper * cosine + lower * sine_part], axis=-1
    )


def segment_masks(block_segments):
    length = block_segments.shape[-1]
    column = jnp.arange(length, dtype=jnp.int32)
    same_segment = block_segments[:, :, None] == block_segments[:, None, :]
    before = column[None, :] < column[:, None]
    positions = jnp.sum((same_segment & before[None]).astype(jnp.int32), axis=2)
    visible = same_segment & (column[None, :] <= column[:, None])[None]
    return (positions, visible)


def join_pieces(mine, theirs, upper_half):
    halves = mine.shape[-1] // 2
    leading = jnp.where(upper_half, theirs, mine)
    trailing = jnp.where(upper_half, mine, theirs)
    return jnp.concatenate(
        [leading[:, :halves], trailing[:, :halves], leading[:, halves:], trailing[:, halves:]],
        axis=-1,
    )


def general_device(hidden, segments, counts, dest_order, norm_gain, q_weight, kv_weight):
    dp_count = lax.axis_size("dp")
    mp_count = lax.axis_size("mp")
    dp_index = lax.axis_index("dp")
    mp_index = lax.axis_index("mp")
    in_slots = segments.shape[0]
    block_len = segments.shape[1]
    kept_slots = in_slots // 2
    per_peer = (in_slots + dp_count - 1) // dp_count
    local_width = hidden.shape[1]
    head_share = max(1, mp_count // KV)
    kv_local = max(1, KV // mp_count)
    token_count = kept_slots * block_len
    device_ids = jnp.arange(dp_count, dtype=jnp.int32)
    starts = jnp.cumsum(counts) - counts
    finishes = starts + counts
    position_of = jnp.sum(
        device_ids[None, :] * (dest_order[None, :] == device_ids[:, None]).astype(jnp.int32), axis=1
    )
    offsets = (position_of - starts[dp_index]) % dp_count
    wanted = offsets[:, None] + jnp.arange(per_peer, dtype=jnp.int32)[None, :] * dp_count
    usable = wanted < counts[dp_index]
    slot_ids = jnp.arange(in_slots, dtype=jnp.int32)
    choose = ((wanted[:, :, None] == slot_ids[None, None, :]) & usable[:, :, None]).astype(
        jnp.bfloat16
    )
    choose = choose.reshape(dp_count * per_peer, in_slots)
    outgoing = jnp.dot(
        choose,
        hidden.reshape(in_slots, block_len * local_width),
        preferred_element_type=jnp.float32,
    ).astype(jnp.bfloat16)
    segment_out = jnp.dot(
        choose, segments.astype(jnp.bfloat16), preferred_element_type=jnp.float32
    ).astype(jnp.bfloat16)
    global_ids = jnp.arange(kept_slots, dtype=jnp.int32) * dp_count + position_of[dp_index]
    sources = jnp.sum((finishes[None, :] <= global_ids[:, None]).astype(jnp.int32), axis=1)
    arrive_rows = sources * per_peer + (global_ids - starts[sources]) // dp_count
    place = (
        arrive_rows[:, None] == jnp.arange(dp_count * per_peer, dtype=jnp.int32)[None, :]
    ).astype(jnp.bfloat16)
    arrived = lax.all_to_all(
        outgoing.reshape(dp_count, per_peer, block_len * local_width),
        "dp",
        split_axis=0,
        concat_axis=0,
        tiled=True,
    )
    segment_in = lax.all_to_all(
        segment_out.reshape(dp_count, per_peer, block_len),
        "dp",
        split_axis=0,
        concat_axis=0,
        tiled=True,
    )
    block_rows = arrived.astype(jnp.float32).reshape(dp_count, per_peer, block_len, local_width)
    arrived_squares = jnp.sum(block_rows * block_rows, axis=3)
    placed_squares = jnp.dot(
        place.astype(jnp.float32),
        arrived_squares.reshape(dp_count * per_peer, block_len),
        precision=lax.Precision.HIGHEST,
    ).reshape(token_count)
    rows = jnp.dot(
        place,
        arrived.reshape(dp_count * per_peer, block_len * local_width),
        preferred_element_type=jnp.float32,
    ).astype(jnp.bfloat16)
    rows = rows.reshape(token_count, local_width)
    block_segments = jnp.dot(
        place,
        segment_in.reshape(dp_count * per_peer, block_len),
        preferred_element_type=jnp.float32,
    )
    widened = rows.astype(jnp.float32)
    totals = lax.psum(placed_squares, "mp")
    row_scale = lax.rsqrt(totals / norm_gain.shape[0] + epsilon)[:, None]
    local_gain = lax.dynamic_slice_in_dim(norm_gain, mp_index * local_width, local_width)
    gained = (widened * local_gain.astype(jnp.float32)).astype(jnp.bfloat16)
    normed = lax.all_gather(gained, "mp", axis=1, tiled=True)
    queries = row_scale * jnp.dot(normed, q_weight, preferred_element_type=jnp.float32)
    kv_rows = (row_scale * jnp.dot(normed, kv_weight, preferred_element_type=jnp.float32)).astype(
        jnp.bfloat16
    )
    for level in range(head_share.bit_length() - 1):
        theirs = swapped(for_sending(kv_rows), "mp", level).astype(kv_rows.dtype)
        upper_half = mp_index // (1 << level) % 2 == 1
        kv_rows = join_pieces(kv_rows, theirs, upper_half)
    kv_split = kv_rows.reshape(token_count, kv_local, 2, HD)
    key_raw = kv_split[:, :, 0, :]
    value_rows = kv_split[:, :, 1, :]
    positions, visible = segment_masks(block_segments)
    cosine, sine_part = rope_tables(positions, HD)
    q_heads = queries.shape[1] // HD
    query_rows = rotate(
        queries.reshape(kept_slots, block_len, q_heads, HD), cosine, sine_part
    ).astype(jnp.bfloat16)
    key_rows = rotate(
        key_raw.astype(jnp.float32).reshape(kept_slots, block_len, kv_local, HD), cosine, sine_part
    ).astype(jnp.bfloat16)
    grouped = query_rows.reshape(kept_slots, block_len, kv_local, q_heads // kv_local, HD)
    scores = jnp.einsum(
        "nikgd,njkd->nkgij", grouped, key_rows, preferred_element_type=jnp.float32
    ) * HD ** (-0.5)
    scores = jnp.where(visible[:, None, None], scores, -jnp.inf)
    highest = jnp.max(scores, axis=-1, keepdims=True)
    weights = jnp.exp(scores - highest)
    shares = (weights / jnp.sum(weights, axis=-1, keepdims=True)).astype(jnp.bfloat16)
    values = value_rows.reshape(kept_slots, block_len, kv_local, HD)
    mixture = jnp.einsum("nkgij,njkd->nikgd", shares, values, preferred_element_type=jnp.float32)
    return mixture.reshape(token_count, q_heads * HD).astype(jnp.bfloat16)


ANY = pl.BlockSpec(memory_space=pl.ANY)
SMEM = pl.BlockSpec(memory_space=pltpu.SMEM)
VMEM = pl.BlockSpec(memory_space=pltpu.VMEM)


def start_of(counts, index, n):
    total = jnp.int32(0)
    for j in range(n):
        total = total + jnp.where(j < index, counts[j], 0)
    return total


def place_of(dest_order, device, n):
    total = jnp.int32(0)
    for j in range(n):
        total = total + jnp.where(dest_order[j] == device, j, 0)
    return total


def pack_kernel(
    counts, dest_order, *refs, n, per_peer, block_len, first, width, rounds, with_ids, in_slots
):
    if with_ids:
        segments, hidden = refs[:2]
        outs = refs[2 : 2 + len(rounds)]
        ids, sems, id_sems = refs[2 + len(rounds) :]
        wide = segments[...].astype(jnp.float32).astype(jnp.bfloat16)
        ids[...] = jnp.broadcast_to(wide[:, None, :], ids.shape)
    else:
        hidden = refs[0]
        outs = refs[1 : 1 + len(rounds)]
        (sems,) = refs[1 + len(rounds) :]
    me = lax.axis_index("dp")
    mine = start_of(counts, me, n)
    copies = []
    for i, r in enumerate(rounds):
        peer = lax.bitwise_xor(me, r)
        offset = lax.rem(place_of(dest_order, peer, n) - mine + n * in_slots, n)
        for a in range(per_peer):
            slot = jnp.minimum(offset + a * n, in_slots - 1)
            row = pl.multiple_of(slot * block_len, block_len)
            copies.append(
                pltpu.make_async_copy(
                    hidden.at[pl.ds(row, block_len), pl.ds(first, width)],
                    outs[i].at[a, pl.ds(0, block_len), :],
                    sems.at[i, a],
                )
            )
            if with_ids:
                copies.append(
                    pltpu.make_async_copy(
                        ids.at[slot],
                        outs[i].at[a, pl.ds(block_len, ID_ROWS), pl.ds(0, block_len)],
                        id_sems.at[i, a],
                    )
                )
    for copy in copies:
        copy.start()
    for copy in copies:
        copy.wait()


def place_kernel(
    counts, dest_order, *refs, n, per_peer, block_len, first, width, groups, with_ids, in_slots
):
    if with_ids:
        sources = refs[:n]
        outs = refs[n : n + len(groups)]
        ids_out = refs[n + len(groups)]
        sems, id_sems = refs[n + len(groups) + 1 :]
    else:
        hidden = refs[0]
        sources = (None,) + tuple(refs[1:n])
        outs = refs[n : n + len(groups)]
        (sems,) = refs[n + len(groups) :]
    me = lax.axis_index("dp")
    my_place = place_of(dest_order, me, n)
    steps = []
    for r in range(n):
        peer = lax.bitwise_xor(me, r)
        begin = start_of(counts, peer, n)
        offset = lax.rem(my_place - begin + n * in_slots, n)
        held = counts[peer]
        for a in range(per_peer):
            slot = offset + a * n
            live = slot < held
            k = lax.div(begin + slot, n)
            if sources[r] is None:
                row = pl.multiple_of(jnp.minimum(slot, in_slots - 1) * block_len, block_len)
                src = hidden.at[pl.ds(row, block_len), pl.ds(first, width)]
            else:
                src = sources[r].at[a, pl.ds(0, block_len), :]
            low = 0
            for g, size in enumerate(groups):
                here = live & (k >= low) & (k < low + size)
                row = pl.multiple_of(jnp.clip(k - low, 0, size - 1) * block_len, block_len)
                steps.append(
                    (
                        here,
                        pltpu.make_async_copy(
                            src, outs[g].at[pl.ds(row, block_len), :], sems.at[r, a]
                        ),
                    )
                )
                low += size
            if with_ids:
                steps.append(
                    (
                        live,
                        pltpu.make_async_copy(
                            sources[r].at[a, pl.ds(block_len, ID_ROWS), pl.ds(0, block_len)],
                            ids_out.at[jnp.clip(k, 0, sum(groups) - 1)],
                            id_sems.at[r, a],
                        ),
                    )
                )
    for here, copy in steps:
        pl.when(here)(copy.start)
    for here, copy in steps:
        pl.when(here)(copy.wait)


def layer_kernel(
    *refs, widths, rows, low, q_heads, kv_local, first_rows, fresh
):
    pieces = refs[: 7 * len(widths)]
    rest = refs[7 * len(widths) :]
    gain, turn, cross, mask, q_weight, kv_weight = rest[:6]
    if fresh:
        out, x, qw, kw, y, stage, sems, weight_sems, out_sem = rest[6:]
    else:
        out, x, qw, kw, y, stage, sems, weight_sems, out_sem = rest[7:]
    me = lax.axis_index("mp")
    local = sum(widths)
    depth = 4 * local
    loads = []
    for m in range(4):
        part = pl.ds(m * local, local)
        loads.append(pltpu.make_async_copy(q_weight.at[part], qw.at[part], weight_sems.at[m, 0]))
        loads.append(pltpu.make_async_copy(kv_weight.at[part], kw.at[part], weight_sems.at[m, 1]))
    steps = []
    begin = 0
    for c, width in enumerate(widths):
        for p in range(7):
            source = me if p == 0 else me - p if p < 4 else me + (p - 3)
            here = (source >= 0) & (source < 4)
            column = pl.multiple_of(jnp.clip(source, 0, 3) * local + begin, 128)
            ref = pieces[c * 7 + p]
            if first_rows[c] is not None:
                ref = ref.at[pl.ds(first_rows[c], rows), :]
            steps.append(
                (
                    here,
                    pltpu.make_async_copy(ref, x.at[:, pl.ds(column, width)], sems.at[c, p]),
                )
            )
        begin += width
    for here, copy in steps:
        pl.when(here)(copy.start)
    for load in loads:
        load.start()
    for here, copy in steps:
        pl.when(here)(copy.wait)
    squares = jnp.zeros((rows, HD), jnp.float32)
    for m in range(4):
        part = slice(m * local, (m + 1) * local)
        raw = x[:, part]
        for t in range(local // HD):
            wide = raw[:, t * HD : (t + 1) * HD].astype(jnp.float32)
            squares = squares + wide * wide
        normed = raw * gain[:, part]
        loads[2 * m].wait()
        loads[2 * m + 1].wait()
        q_part = jnp.dot(normed, qw[part, :], preferred_element_type=jnp.float32)
        kv_part = jnp.dot(normed, kw[part, :], preferred_element_type=jnp.float32)
        if m == 0:
            y[:, : q_heads * HD] = q_part
            y[:, q_heads * HD :] = kv_part
        else:
            y[:, : q_heads * HD] += q_part
            y[:, q_heads * HD :] += kv_part
    scale = lax.rsqrt(jnp.sum(squares, axis=1, keepdims=True) / depth + epsilon)
    per_kv = q_heads // kv_local
    length = mask.shape[1]
    for b in range(rows // length):
        here = slice(b * length, (b + 1) * length)
        row_scale = scale[here]
        cosine = turn[here, :]
        sine = cross[here, :]
        visible = mask[here, :] > 0

        def rotated(value):
            return (value * cosine + pltpu.roll(value, HD // 2, 1) * sine).astype(jnp.bfloat16)

        visible_all = jnp.concatenate([visible] * per_kv, axis=0)
        for j in range(kv_local):
            base = q_heads * HD + 2 * j * HD
            key = (row_scale * y[here, base : base + HD]).astype(jnp.bfloat16)
            key = rotated(key.astype(jnp.float32))
            value = (row_scale * y[here, base + HD : base + 2 * HD]).astype(jnp.bfloat16)
            query = jnp.concatenate(
                [
                    rotated(row_scale * y[here, h * HD : (h + 1) * HD])
                    for h in range(j * per_kv, (j + 1) * per_kv)
                ],
                axis=0,
            )
            scores = lax.dot_general(
                query, key, (((1,), (1,)), ((), ())), preferred_element_type=jnp.float32
            ) * HD ** (-0.5)
            scores = jnp.where(visible_all, scores, -jnp.inf)
            highest = jnp.max(scores, axis=1, keepdims=True)
            weights = jnp.exp(scores - highest)
            shares = (weights / jnp.sum(weights, axis=1, keepdims=True)).astype(jnp.bfloat16)
            mixed = jnp.dot(shares, value, preferred_element_type=jnp.float32).astype(jnp.bfloat16)
            for i in range(per_kv):
                h = j * per_kv + i
                stage[here, h * HD : (h + 1) * HD] = mixed[i * length : (i + 1) * length]
    copy = pltpu.make_async_copy(stage, out.at[pl.ds(low, rows), :], out_sem)
    copy.start()
    copy.wait()


def line_device(hidden, segments, counts, dest_order, norm_gain, q_weight, kv_weight):
    n = lax.axis_size("dp")
    in_slots, block_len = segments.shape
    kept = in_slots // 2
    per_peer = (in_slots + n - 1) // n
    local = hidden.shape[1]
    tokens = kept * block_len
    q_heads = q_weight.shape[1] // HD
    kv_local = kv_weight.shape[1] // (2 * HD)
    bf16 = jnp.bfloat16
    widths = tuple(local * e // 8 for e in FEATURE_EIGHTHS)
    dma = pltpu.SemaphoreType.DMA
    own, arrived = [], []
    first = 0
    exchanged = []
    for c, width in enumerate(widths):
        rounds = tuple(range(n)) if c == 0 else tuple(range(1, n))
        height = block_len + (ID_ROWS if c == 0 else 0)
        kernel = functools.partial(
            pack_kernel,
            n=n,
            per_peer=per_peer,
            block_len=block_len,
            first=first,
            width=width,
            rounds=rounds,
            with_ids=c == 0,
            in_slots=in_slots,
        )
        scratch = [dma((len(rounds), per_peer))]
        if c == 0:
            scratch = [pltpu.VMEM((in_slots, ID_ROWS, block_len), bf16)] + scratch * 2
        packed = pl.pallas_call(
            kernel,
            out_shape=[jax.ShapeDtypeStruct((per_peer, height, width), bf16)] * len(rounds),
            in_specs=[SMEM, SMEM] + ([VMEM] if c == 0 else []) + [ANY],
            out_specs=[ANY] * len(rounds),
            scratch_shapes=scratch,
            name=f"pack{c}",
        )(counts, dest_order, *((segments,) if c == 0 else ()), hidden)
        came = []
        for r, buffer in zip(rounds, packed):
            if r == 0:
                came.append(buffer)
            else:
                pairs = [(s, s ^ r) for s in range(n)]
                came.append(lax.ppermute(buffer, "dp", pairs))
        exchanged.append((first, width, came))
        first += width
    right = [(0, 1), (1, 2), (2, 3)]
    left = [(1, 0), (2, 1), (3, 2)]

    def along(value):
        r1 = lax.ppermute(value, "mp", right)
        l1 = lax.ppermute(value, "mp", left)
        r2 = lax.ppermute(r1, "mp", right[1:])
        l2 = lax.ppermute(l1, "mp", left[:2])
        r3 = lax.ppermute(r2, "mp", right[2:])
        l3 = lax.ppermute(l2, "mp", left[:1])
        return [value, r1, r2, r3, l1, l2, l3]

    gathered = []
    block_ids = None
    for c, (first, width, came) in enumerate(exchanged):
        groups = (kept,) if c == 0 else GROUPS
        kernel = functools.partial(
            place_kernel,
            n=n,
            per_peer=per_peer,
            block_len=block_len,
            first=first,
            width=width,
            groups=groups,
            with_ids=c == 0,
            in_slots=in_slots,
        )
        shapes = [jax.ShapeDtypeStruct((size * block_len, width), bf16) for size in groups]
        scratch = [dma((n, per_peer))]
        if c == 0:
            shapes.append(jax.ShapeDtypeStruct((kept, ID_ROWS, block_len), bf16))
            scratch = scratch * 2
        placed = pl.pallas_call(
            kernel,
            out_shape=shapes,
            in_specs=[SMEM, SMEM] + [ANY] * n,
            out_specs=[ANY] * len(shapes),
            scratch_shapes=scratch,
            name=f"place{c}",
        )(counts, dest_order, *(() if c == 0 else (hidden,)), *came)
        if c == 0:
            block_ids = placed[-1][:, 0, :]
            placed = placed[:-1]
        gathered.append([along(piece) for piece in placed])
    positions, visible = segment_masks(block_ids)
    cosine, sine = rope_tables(positions, HD)
    turn = jnp.concatenate([cosine, cosine], axis=-1).reshape(tokens, HD)
    cross = jnp.concatenate([-sine, sine], axis=-1).reshape(tokens, HD)
    mask = visible.astype(jnp.float32).reshape(tokens, block_len)
    gain = norm_gain[None, :]
    out = None
    low = 0
    for g, size in enumerate(GROUPS):
        rows = size * block_len
        pieces, first_rows = [], []
        for c in range(len(widths)):
            whole = len(gathered[c]) == 1
            pieces += gathered[c][0 if whole else g]
            first_rows.append(low if whole else None)
        kernel = functools.partial(
            layer_kernel,
            widths=widths,
            rows=rows,
            low=low,
            q_heads=q_heads,
            kv_local=kv_local,
            first_rows=tuple(first_rows),
            fresh=out is None,
        )
        part = slice(low, low + rows)
        operands = pieces + [gain, turn[part], cross[part], mask[part], q_weight, kv_weight]
        specs = [ANY] * len(pieces) + [VMEM] * 4 + [ANY] * 2
        aliases = {}
        if out is not None:
            aliases = {len(operands): 0}
            operands.append(out)
            specs.append(ANY)
        flops = 2 * rows * q_weight.shape[0] * (q_weight.shape[1] + kv_weight.shape[1])
        out = pl.pallas_call(
            kernel,
            out_shape=jax.ShapeDtypeStruct((tokens, q_heads * HD), bf16),
            in_specs=specs,
            out_specs=ANY,
            input_output_aliases=aliases,
            scratch_shapes=[
                pltpu.VMEM((rows, 4 * local), bf16),
                pltpu.VMEM(q_weight.shape, bf16),
                pltpu.VMEM(kv_weight.shape, bf16),
                pltpu.VMEM((rows, q_weight.shape[1] + kv_weight.shape[1]), jnp.float32),
                pltpu.VMEM((rows, q_heads * HD), bf16),
                dma((len(widths), 7)),
                dma((4, 2)),
                dma(()),
            ],
            compiler_params=pltpu.CompilerParams(vmem_limit_bytes=48 * 1024 * 1024),
            cost_estimate=pl.CostEstimate(
                flops=flops, transcendentals=0, bytes_accessed=16 * 1024 * 1024
            ),
            name=f"layer{g}",
        )(*operands)
        low += rows
    return out


def solution(mesh):
    in_specs = (P("dp", "mp"), P("dp", None), P(), P(), P(), P(None, "mp"), P(None, "mp"))
    out_specs = P("dp", "mp")
    dp_count, mp_count = mesh.shape["dp"], mesh.shape["mp"]
    line = mp_count == 4 and KV % mp_count == 0 and dp_count & (dp_count - 1) == 0
    return jax.shard_map(
        line_device if line else general_device,
        mesh=mesh,
        in_specs=in_specs,
        out_specs=out_specs,
        check_vma=False,
    )
```

```python
import functools

import jax
import jax.numpy as jnp
from jax import lax
from jax.experimental import pallas as pl
from jax.experimental.pallas import tpu as pltpu
from jax.sharding import PartitionSpec as P

KV = 8
HD = 128


epsilon = 1e-05
rope_base = 500000.0

ID_ROWS = 8
FEATURE_EIGHTHS = (2, 6)
GROUPS = (2, 2, 2, 2)


def for_sending(array):
    return jax.tree.map(lambda a: a.astype(jnp.bfloat16) if a.dtype == jnp.float32 else a, array)


def swapped(value, axis, stride):
    mask = 2**stride
    pairs = [(source, source ^ mask) for source in range(lax.axis_size(axis))]
    return lax.ppermute(value, axis, pairs)


def rope_tables(positions, width):
    halves = width // 2
    frequency = rope_base ** (-(jnp.arange(halves, dtype=jnp.float32) * 2.0) / width)
    angles = positions.astype(jnp.float32)[..., None] * frequency
    return (jnp.cos(angles), jnp.sin(angles))


def rotate(tensor, cosine, sine_part):
    halves = tensor.shape[-1] // 2
    lower = tensor[..., :halves]
    upper = tensor[..., halves:]
    cosine = cosine[..., None, :]
    sine_part = sine_part[..., None, :]
    return jnp.concatenate(
        [lower * cosine - upper * sine_part, upper * cosine + lower * sine_part], axis=-1
    )


def segment_masks(block_segments):
    length = block_segments.shape[-1]
    column = jnp.arange(length, dtype=jnp.int32)
    same_segment = block_segments[:, :, None] == block_segments[:, None, :]
    before = column[None, :] < column[:, None]
    positions = jnp.sum((same_segment & before[None]).astype(jnp.int32), axis=2)
    visible = same_segment & (column[None, :] <= column[:, None])[None]
    return (positions, visible)


def join_pieces(mine, theirs, upper_half):
    halves = mine.shape[-1] // 2
    leading = jnp.where(upper_half, theirs, mine)
    trailing = jnp.where(upper_half, mine, theirs)
    return jnp.concatenate(
        [leading[:, :halves], trailing[:, :halves], leading[:, halves:], trailing[:, halves:]],
        axis=-1,
    )


def general_device(hidden, segments, counts, dest_order, norm_gain, q_weight, kv_weight):
    dp_count = lax.axis_size("dp")
    mp_count = lax.axis_size("mp")
    dp_index = lax.axis_index("dp")
    mp_index = lax.axis_index("mp")
    in_slots = segments.shape[0]
    block_len = segments.shape[1]
    kept_slots = in_slots // 2
    per_peer = (in_slots + dp_count - 1) // dp_count
    local_width = hidden.shape[1]
    head_share = max(1, mp_count // KV)
    kv_local = max(1, KV // mp_count)
    token_count = kept_slots * block_len
    device_ids = jnp.arange(dp_count, dtype=jnp.int32)
    starts = jnp.cumsum(counts) - counts
    finishes = starts + counts
    position_of = jnp.sum(
        device_ids[None, :] * (dest_order[None, :] == device_ids[:, None]).astype(jnp.int32), axis=1
    )
    offsets = (position_of - starts[dp_index]) % dp_count
    wanted = offsets[:, None] + jnp.arange(per_peer, dtype=jnp.int32)[None, :] * dp_count
    usable = wanted < counts[dp_index]
    slot_ids = jnp.arange(in_slots, dtype=jnp.int32)
    choose = ((wanted[:, :, None] == slot_ids[None, None, :]) & usable[:, :, None]).astype(
        jnp.bfloat16
    )
    choose = choose.reshape(dp_count * per_peer, in_slots)
    outgoing = jnp.dot(
        choose,
        hidden.reshape(in_slots, block_len * local_width),
        preferred_element_type=jnp.float32,
    ).astype(jnp.bfloat16)
    segment_out = jnp.dot(
        choose, segments.astype(jnp.bfloat16), preferred_element_type=jnp.float32
    ).astype(jnp.bfloat16)
    global_ids = jnp.arange(kept_slots, dtype=jnp.int32) * dp_count + position_of[dp_index]
    sources = jnp.sum((finishes[None, :] <= global_ids[:, None]).astype(jnp.int32), axis=1)
    arrive_rows = sources * per_peer + (global_ids - starts[sources]) // dp_count
    place = (
        arrive_rows[:, None] == jnp.arange(dp_count * per_peer, dtype=jnp.int32)[None, :]
    ).astype(jnp.bfloat16)
    arrived = lax.all_to_all(
        outgoing.reshape(dp_count, per_peer, block_len * local_width),
        "dp",
        split_axis=0,
        concat_axis=0,
        tiled=True,
    )
    segment_in = lax.all_to_all(
        segment_out.reshape(dp_count, per_peer, block_len),
        "dp",
        split_axis=0,
        concat_axis=0,
        tiled=True,
    )
    block_rows = arrived.astype(jnp.float32).reshape(dp_count, per_peer, block_len, local_width)
    arrived_squares = jnp.sum(block_rows * block_rows, axis=3)
    placed_squares = jnp.dot(
        place.astype(jnp.float32),
        arrived_squares.reshape(dp_count * per_peer, block_len),
        precision=lax.Precision.HIGHEST,
    ).reshape(token_count)
    rows = jnp.dot(
        place,
        arrived.reshape(dp_count * per_peer, block_len * local_width),
        preferred_element_type=jnp.float32,
    ).astype(jnp.bfloat16)
    rows = rows.reshape(token_count, local_width)
    block_segments = jnp.dot(
        place,
        segment_in.reshape(dp_count * per_peer, block_len),
        preferred_element_type=jnp.float32,
    )
    widened = rows.astype(jnp.float32)
    totals = lax.psum(placed_squares, "mp")
    row_scale = lax.rsqrt(totals / norm_gain.shape[0] + epsilon)[:, None]
    local_gain = lax.dynamic_slice_in_dim(norm_gain, mp_index * local_width, local_width)
    gained = (widened * local_gain.astype(jnp.float32)).astype(jnp.bfloat16)
    normed = lax.all_gather(gained, "mp", axis=1, tiled=True)
    queries = row_scale * jnp.dot(normed, q_weight, preferred_element_type=jnp.float32)
    kv_rows = (row_scale * jnp.dot(normed, kv_weight, preferred_element_type=jnp.float32)).astype(
        jnp.bfloat16
    )
    for level in range(head_share.bit_length() - 1):
        theirs = swapped(for_sending(kv_rows), "mp", level).astype(kv_rows.dtype)
        upper_half = mp_index // (1 << level) % 2 == 1
        kv_rows = join_pieces(kv_rows, theirs, upper_half)
    kv_split = kv_rows.reshape(token_count, kv_local, 2, HD)
    key_raw = kv_split[:, :, 0, :]
    value_rows = kv_split[:, :, 1, :]
    positions, visible = segment_masks(block_segments)
    cosine, sine_part = rope_tables(positions, HD)
    q_heads = queries.shape[1] // HD
    query_rows = rotate(
        queries.reshape(kept_slots, block_len, q_heads, HD), cosine, sine_part
    ).astype(jnp.bfloat16)
    key_rows = rotate(
        key_raw.astype(jnp.float32).reshape(kept_slots, block_len, kv_local, HD), cosine, sine_part
    ).astype(jnp.bfloat16)
    grouped = query_rows.reshape(kept_slots, block_len, kv_local, q_heads // kv_local, HD)
    scores = jnp.einsum(
        "nikgd,njkd->nkgij", grouped, key_rows, preferred_element_type=jnp.float32
    ) * HD ** (-0.5)
    scores = jnp.where(visible[:, None, None], scores, -jnp.inf)
    highest = jnp.max(scores, axis=-1, keepdims=True)
    weights = jnp.exp(scores - highest)
    shares = (weights / jnp.sum(weights, axis=-1, keepdims=True)).astype(jnp.bfloat16)
    values = value_rows.reshape(kept_slots, block_len, kv_local, HD)
    mixture = jnp.einsum("nkgij,njkd->nikgd", shares, values, preferred_element_type=jnp.float32)
    return mixture.reshape(token_count, q_heads * HD).astype(jnp.bfloat16)


ANY = pl.BlockSpec(memory_space=pl.ANY)
SMEM = pl.BlockSpec(memory_space=pltpu.SMEM)
VMEM = pl.BlockSpec(memory_space=pltpu.VMEM)


def start_of(counts, index, n):
    total = jnp.int32(0)
    for j in range(n):
        total = total + jnp.where(j < index, counts[j], 0)
    return total


def place_of(dest_order, device, n):
    total = jnp.int32(0)
    for j in range(n):
        total = total + jnp.where(dest_order[j] == device, j, 0)
    return total


def pack_kernel(counts, dest_order, segments, hidden, *refs, n, per_peer, block_len, widths):
    outs = refs[: len(widths)]
    (sems,) = refs[len(widths) :]
    in_slots = segments.shape[0]
    me = lax.axis_index("dp")
    mine = start_of(counts, me, n)
    copies = []
    begin = 0
    for c, width in enumerate(widths):
        for peer in range(n):
            offset = lax.rem(place_of(dest_order, peer, n) - mine + n * in_slots, n)
            for a in range(per_peer):
                slot = jnp.minimum(offset + a * n, in_slots - 1)
                row = pl.multiple_of(slot * block_len, block_len)
                copies.append(
                    pltpu.make_async_copy(
                        hidden.at[pl.ds(row, block_len), pl.ds(begin, width)],
                        outs[c].at[peer, a, pl.ds(0, block_len), :],
                        sems.at[c, peer, a],
                    )
                )
                copies[-1].start()
                if c == 0:
                    ids = segments[pl.ds(slot, 1), :].astype(jnp.float32)
                    ids = jnp.broadcast_to(ids, (ID_ROWS, block_len)).astype(jnp.bfloat16)
                    outs[0][peer, a, block_len:, :block_len] = ids
        begin += width
    for copy in copies:
        copy.wait()


def place_kernel(counts, dest_order, arrived, *outs, n, block_len, groups, with_ids):
    me = lax.axis_index("dp")
    my_place = place_of(dest_order, me, n)
    k = 0
    for g, size in enumerate(groups):
        for i in range(size):
            wanted = k * n + my_place
            source = jnp.int32(0)
            begin = jnp.int32(0)
            total = jnp.int32(0)
            for j in range(n):
                total = total + counts[j]
                passed = total <= wanted
                source = source + passed.astype(jnp.int32)
                begin = jnp.where(passed, total, begin)
            a = lax.div(wanted - begin, n)
            outs[g][i * block_len : (i + 1) * block_len, :] = arrived[source, a, :block_len, :]
            if with_ids:
                outs[-1][k] = arrived[source, a, block_len:, :block_len]
            k += 1


def layer_kernel(*refs, widths, rows, low, q_heads, kv_local, first_rows, fresh):
    count = len(widths)
    pieces = refs[: 6 * count]
    gain, turn, cross, mask, q_weight, kv_weight = refs[6 * count : 6 * count + 6]
    out, x, y, stage, out_sem = refs[6 * count + (6 if fresh else 7) :]
    me = lax.axis_index("mp")
    inner = (me == 1) | (me == 2)
    local = sum(widths)
    depth = 4 * local
    begin = 0
    for c, width in enumerate(widths):
        own, near, mid, far, end_mid, end_far = pieces[6 * c : 6 * c + 6]
        row = slice(None) if first_rows[c] is None else slice(first_rows[c], first_rows[c] + rows)
        pair = lax.bitwise_xor(me, 1)
        second = jnp.where(inner, 3 - me, jnp.where(me == 0, 2, 1))
        third = jnp.where(inner, lax.bitwise_xor(3 - me, 1), 3 - me)

        def put(source, value):
            column = pl.multiple_of(source * local + begin, HD)
            x[:, pl.ds(column, width)] = value

        put(me, own[row, :])
        put(pair, near[row, :])

        @pl.when(inner)
        def _():
            put(second, mid[row, :])
            put(third, far[row, :])

        @pl.when(jnp.logical_not(inner))
        def _():
            put(second, end_mid[row, :])
            put(third, end_far[row, :])

        begin += width
    squares = jnp.zeros((rows, HD), jnp.float32)
    for m in range(4):
        part = slice(m * local, (m + 1) * local)
        raw = x[:, part]
        for t in range(local // HD):
            wide = raw[:, t * HD : (t + 1) * HD].astype(jnp.float32)
            squares = squares + wide * wide
        x[:, part] = raw * gain[:, part]
    scale = lax.rsqrt(jnp.sum(squares, axis=1, keepdims=True) / depth + epsilon)
    normed = x[...]
    y[:, : q_heads * HD] = jnp.dot(normed, q_weight[...], preferred_element_type=jnp.float32)
    y[:, q_heads * HD :] = jnp.dot(normed, kv_weight[...], preferred_element_type=jnp.float32)
    per_kv = q_heads // kv_local
    length = mask.shape[1]
    for b in range(rows // length):
        here = slice(b * length, (b + 1) * length)
        row_scale = scale[here]
        cosine = turn[here, :]
        sine = cross[here, :]
        visible = mask[here, :] > 0

        def rotated(value):
            return (value * cosine + pltpu.roll(value, HD // 2, 1) * sine).astype(jnp.bfloat16)

        visible_all = jnp.concatenate([visible] * per_kv, axis=0)
        for j in range(kv_local):
            base = q_heads * HD + 2 * j * HD
            key = (row_scale * y[here, base : base + HD]).astype(jnp.bfloat16)
            key = rotated(key.astype(jnp.float32))
            value = (row_scale * y[here, base + HD : base + 2 * HD]).astype(jnp.bfloat16)
            query = jnp.concatenate(
                [
                    rotated(row_scale * y[here, h * HD : (h + 1) * HD])
                    for h in range(j * per_kv, (j + 1) * per_kv)
                ],
                axis=0,
            )
            scores = lax.dot_general(
                query, key, (((1,), (1,)), ((), ())), preferred_element_type=jnp.float32
            ) * HD ** (-0.5)
            scores = jnp.where(visible_all, scores, -jnp.inf)
            highest = jnp.max(scores, axis=1, keepdims=True)
            weights = jnp.exp(scores - highest)
            shares = (weights / jnp.sum(weights, axis=1, keepdims=True)).astype(jnp.bfloat16)
            mixed = jnp.dot(shares, value, preferred_element_type=jnp.float32).astype(jnp.bfloat16)
            for i in range(per_kv):
                h = j * per_kv + i
                stage[here, h * HD : (h + 1) * HD] = mixed[i * length : (i + 1) * length]
    copy = pltpu.make_async_copy(stage, out.at[pl.ds(low, rows), :], out_sem)
    copy.start()
    copy.wait()


PAIRS = [(0, 1), (1, 0), (2, 3), (3, 2)]
MIDDLE = [(1, 2), (2, 1)]
OUTWARD = [(1, 0), (2, 3)]


def send(value, pairs):
    return lax.ppermute(value, "mp", pairs)


def line_device(hidden, segments, counts, dest_order, norm_gain, q_weight, kv_weight):
    n = lax.axis_size("dp")
    in_slots, block_len = segments.shape
    kept = in_slots // 2
    per_peer = (in_slots + n - 1) // n
    local = hidden.shape[1]
    tokens = kept * block_len
    q_heads = q_weight.shape[1] // HD
    kv_local = kv_weight.shape[1] // (2 * HD)
    bf16 = jnp.bfloat16
    widths = tuple(local * e // 8 for e in FEATURE_EIGHTHS)
    dma = pltpu.SemaphoreType.DMA
    heights = [block_len + (ID_ROWS if c == 0 else 0) for c in range(len(widths))]
    packed = pl.pallas_call(
        functools.partial(
            pack_kernel, n=n, per_peer=per_peer, block_len=block_len, widths=widths
        ),
        out_shape=[
            jax.ShapeDtypeStruct((n, per_peer, height, width), bf16)
            for height, width in zip(heights, widths)
        ],
        in_specs=[SMEM, SMEM, VMEM, ANY],
        out_specs=[VMEM] * len(widths),
        scratch_shapes=[dma((len(widths), n, per_peer))],
        name="pack",
    )(counts, dest_order, segments, hidden)
    came = []
    for buffer in packed:
        came.append(lax.all_to_all(buffer, "dp", split_axis=0, concat_axis=0, tiled=True))
    gathered = []
    block_ids = None
    for c, (width, arrived) in enumerate(zip(widths, came)):
        groups = (kept,) if c == 0 else GROUPS
        shapes = [jax.ShapeDtypeStruct((size * block_len, width), bf16) for size in groups]
        if c == 0:
            shapes.append(jax.ShapeDtypeStruct((kept, ID_ROWS, block_len), bf16))
        placed = pl.pallas_call(
            functools.partial(
                place_kernel, n=n, block_len=block_len, groups=groups, with_ids=c == 0
            ),
            out_shape=shapes,
            in_specs=[SMEM, SMEM, VMEM],
            out_specs=[VMEM] * len(shapes),
        )(counts, dest_order, arrived)
        if c == 0:
            block_ids = placed[-1][:, 0, :]
            placed = placed[:-1]
        rows = []
        for own in placed:
            near = send(own, PAIRS)
            mid = send(own, MIDDLE)
            far = send(near, MIDDLE)
            end_mid = send(mid, OUTWARD)
            end_far = send(far, OUTWARD)
            rows.append([own, near, mid, far, end_mid, end_far])
        gathered.append(rows)
    positions, visible = segment_masks(block_ids)
    cosine, sine = rope_tables(positions, HD)
    turn = jnp.concatenate([cosine, cosine], axis=-1).reshape(tokens, HD)
    cross = jnp.concatenate([-sine, sine], axis=-1).reshape(tokens, HD)
    mask = visible.astype(jnp.float32).reshape(tokens, block_len)
    gain = norm_gain[None, :]
    out = None
    low = 0
    for g, size in enumerate(GROUPS):
        rows = size * block_len
        pieces, first_rows = [], []
        for c in range(len(widths)):
            whole = len(gathered[c]) == 1
            pieces += gathered[c][0 if whole else g]
            first_rows.append(low if whole else None)
        kernel = functools.partial(
            layer_kernel,
            widths=widths,
            rows=rows,
            low=low,
            q_heads=q_heads,
            kv_local=kv_local,
            first_rows=tuple(first_rows),
            fresh=out is None,
        )
        part = slice(low, low + rows)
        operands = pieces + [gain, turn[part], cross[part], mask[part], q_weight, kv_weight]
        specs = [VMEM] * len(operands)
        aliases = {}
        if out is not None:
            aliases = {len(operands): 0}
            operands.append(out)
            specs.append(ANY)
        flops = 2 * rows * q_weight.shape[0] * (q_weight.shape[1] + kv_weight.shape[1])
        out = pl.pallas_call(
            kernel,
            out_shape=jax.ShapeDtypeStruct((tokens, q_heads * HD), bf16),
            in_specs=specs,
            out_specs=ANY,
            input_output_aliases=aliases,
            scratch_shapes=[
                pltpu.VMEM((rows, 4 * local), bf16),
                pltpu.VMEM((rows, q_weight.shape[1] + kv_weight.shape[1]), jnp.float32),
                pltpu.VMEM((rows, q_heads * HD), bf16),
                dma(()),
            ],
            cost_estimate=pl.CostEstimate(
                flops=flops, transcendentals=0, bytes_accessed=16 * 1024 * 1024
            ),
        )(*operands)
        low += rows
    return out


def solution(mesh):
    in_specs = (P("dp", "mp"), P("dp", None), P(), P(), P(), P(None, "mp"), P(None, "mp"))
    out_specs = P("dp", "mp")
    mp_count = mesh.shape["mp"]
    line = mp_count == 4 and KV % mp_count == 0

    def body(*arrays):
        return line_device(*arrays)

    return jax.shard_map(
        body if line else general_device,
        mesh=mesh,
        in_specs=in_specs,
        out_specs=out_specs,
        check_vma=False,
    )
```

```python
import functools

import jax
import jax.numpy as jnp
import numpy as np
from jax import lax
from jax.experimental import pallas as pl
from jax.experimental.pallas import tpu as pltpu
from jax.sharding import PartitionSpec as P

KV = 8
HD = 128


epsilon = 1e-05
rope_base = 500000.0

ID_ROWS = 8
FEATURE_EIGHTHS = (3, 5)
GROUPS = (3, 2, 2, 1)


def for_sending(array):
    return jax.tree.map(lambda a: a.astype(jnp.bfloat16) if a.dtype == jnp.float32 else a, array)


def swapped(value, axis, stride):
    mask = 2**stride
    pairs = [(source, source ^ mask) for source in range(lax.axis_size(axis))]
    return lax.ppermute(value, axis, pairs)


def rope_tables(positions, width):
    halves = width // 2
    frequency = rope_base ** (-(jnp.arange(halves, dtype=jnp.float32) * 2.0) / width)
    angles = positions.astype(jnp.float32)[..., None] * frequency
    return (jnp.cos(angles), jnp.sin(angles))


def rotate(tensor, cosine, sine_part):
    halves = tensor.shape[-1] // 2
    lower = tensor[..., :halves]
    upper = tensor[..., halves:]
    cosine = cosine[..., None, :]
    sine_part = sine_part[..., None, :]
    return jnp.concatenate(
        [lower * cosine - upper * sine_part, upper * cosine + lower * sine_part], axis=-1
    )


def segment_masks(block_segments):
    length = block_segments.shape[-1]
    column = jnp.arange(length, dtype=jnp.int32)
    same_segment = block_segments[:, :, None] == block_segments[:, None, :]
    before = column[None, :] < column[:, None]
    positions = jnp.sum((same_segment & before[None]).astype(jnp.int32), axis=2)
    visible = same_segment & (column[None, :] <= column[:, None])[None]
    return (positions, visible)


def join_pieces(mine, theirs, upper_half):
    halves = mine.shape[-1] // 2
    leading = jnp.where(upper_half, theirs, mine)
    trailing = jnp.where(upper_half, mine, theirs)
    return jnp.concatenate(
        [leading[:, :halves], trailing[:, :halves], leading[:, halves:], trailing[:, halves:]],
        axis=-1,
    )


def general_device(hidden, segments, counts, dest_order, norm_gain, q_weight, kv_weight):
    dp_count = lax.axis_size("dp")
    mp_count = lax.axis_size("mp")
    dp_index = lax.axis_index("dp")
    mp_index = lax.axis_index("mp")
    in_slots = segments.shape[0]
    block_len = segments.shape[1]
    kept_slots = in_slots // 2
    per_peer = (in_slots + dp_count - 1) // dp_count
    local_width = hidden.shape[1]
    head_share = max(1, mp_count // KV)
    kv_local = max(1, KV // mp_count)
    token_count = kept_slots * block_len
    device_ids = jnp.arange(dp_count, dtype=jnp.int32)
    starts = jnp.cumsum(counts) - counts
    finishes = starts + counts
    position_of = jnp.sum(
        device_ids[None, :] * (dest_order[None, :] == device_ids[:, None]).astype(jnp.int32), axis=1
    )
    offsets = (position_of - starts[dp_index]) % dp_count
    wanted = offsets[:, None] + jnp.arange(per_peer, dtype=jnp.int32)[None, :] * dp_count
    usable = wanted < counts[dp_index]
    slot_ids = jnp.arange(in_slots, dtype=jnp.int32)
    choose = ((wanted[:, :, None] == slot_ids[None, None, :]) & usable[:, :, None]).astype(
        jnp.bfloat16
    )
    choose = choose.reshape(dp_count * per_peer, in_slots)
    outgoing = jnp.dot(
        choose,
        hidden.reshape(in_slots, block_len * local_width),
        preferred_element_type=jnp.float32,
    ).astype(jnp.bfloat16)
    segment_out = jnp.dot(
        choose, segments.astype(jnp.bfloat16), preferred_element_type=jnp.float32
    ).astype(jnp.bfloat16)
    global_ids = jnp.arange(kept_slots, dtype=jnp.int32) * dp_count + position_of[dp_index]
    sources = jnp.sum((finishes[None, :] <= global_ids[:, None]).astype(jnp.int32), axis=1)
    arrive_rows = sources * per_peer + (global_ids - starts[sources]) // dp_count
    place = (
        arrive_rows[:, None] == jnp.arange(dp_count * per_peer, dtype=jnp.int32)[None, :]
    ).astype(jnp.bfloat16)
    arrived = lax.all_to_all(
        outgoing.reshape(dp_count, per_peer, block_len * local_width),
        "dp",
        split_axis=0,
        concat_axis=0,
        tiled=True,
    )
    segment_in = lax.all_to_all(
        segment_out.reshape(dp_count, per_peer, block_len),
        "dp",
        split_axis=0,
        concat_axis=0,
        tiled=True,
    )
    block_rows = arrived.astype(jnp.float32).reshape(dp_count, per_peer, block_len, local_width)
    arrived_squares = jnp.sum(block_rows * block_rows, axis=3)
    placed_squares = jnp.dot(
        place.astype(jnp.float32),
        arrived_squares.reshape(dp_count * per_peer, block_len),
        precision=lax.Precision.HIGHEST,
    ).reshape(token_count)
    rows = jnp.dot(
        place,
        arrived.reshape(dp_count * per_peer, block_len * local_width),
        preferred_element_type=jnp.float32,
    ).astype(jnp.bfloat16)
    rows = rows.reshape(token_count, local_width)
    block_segments = jnp.dot(
        place,
        segment_in.reshape(dp_count * per_peer, block_len),
        preferred_element_type=jnp.float32,
    )
    widened = rows.astype(jnp.float32)
    totals = lax.psum(placed_squares, "mp")
    row_scale = lax.rsqrt(totals / norm_gain.shape[0] + epsilon)[:, None]
    local_gain = lax.dynamic_slice_in_dim(norm_gain, mp_index * local_width, local_width)
    gained = (widened * local_gain.astype(jnp.float32)).astype(jnp.bfloat16)
    normed = lax.all_gather(gained, "mp", axis=1, tiled=True)
    queries = row_scale * jnp.dot(normed, q_weight, preferred_element_type=jnp.float32)
    kv_rows = (row_scale * jnp.dot(normed, kv_weight, preferred_element_type=jnp.float32)).astype(
        jnp.bfloat16
    )
    for level in range(head_share.bit_length() - 1):
        theirs = swapped(for_sending(kv_rows), "mp", level).astype(kv_rows.dtype)
        upper_half = mp_index // (1 << level) % 2 == 1
        kv_rows = join_pieces(kv_rows, theirs, upper_half)
    kv_split = kv_rows.reshape(token_count, kv_local, 2, HD)
    key_raw = kv_split[:, :, 0, :]
    value_rows = kv_split[:, :, 1, :]
    positions, visible = segment_masks(block_segments)
    cosine, sine_part = rope_tables(positions, HD)
    q_heads = queries.shape[1] // HD
    query_rows = rotate(
        queries.reshape(kept_slots, block_len, q_heads, HD), cosine, sine_part
    ).astype(jnp.bfloat16)
    key_rows = rotate(
        key_raw.astype(jnp.float32).reshape(kept_slots, block_len, kv_local, HD), cosine, sine_part
    ).astype(jnp.bfloat16)
    grouped = query_rows.reshape(kept_slots, block_len, kv_local, q_heads // kv_local, HD)
    scores = jnp.einsum(
        "nikgd,njkd->nkgij", grouped, key_rows, preferred_element_type=jnp.float32
    ) * HD ** (-0.5)
    scores = jnp.where(visible[:, None, None], scores, -jnp.inf)
    highest = jnp.max(scores, axis=-1, keepdims=True)
    weights = jnp.exp(scores - highest)
    shares = (weights / jnp.sum(weights, axis=-1, keepdims=True)).astype(jnp.bfloat16)
    values = value_rows.reshape(kept_slots, block_len, kv_local, HD)
    mixture = jnp.einsum("nkgij,njkd->nikgd", shares, values, preferred_element_type=jnp.float32)
    return mixture.reshape(token_count, q_heads * HD).astype(jnp.bfloat16)


ANY = pl.BlockSpec(memory_space=pl.ANY)
SMEM = pl.BlockSpec(memory_space=pltpu.SMEM)
VMEM = pl.BlockSpec(memory_space=pltpu.VMEM)
MIB = 1024 * 1024


def resident(value):
    return pltpu.with_memory_space_constraint(value, pltpu.VMEM)


def afar(value):
    return pltpu.with_memory_space_constraint(value, pltpu.HBM)


def limit(mib):
    return pltpu.CompilerParams(vmem_limit_bytes=mib * MIB)


def start_of(counts, index, n):
    total = jnp.int32(0)
    for j in range(n):
        total = total + jnp.where(j < index, counts[j], 0)
    return total


def place_of(dest_order, device, n):
    total = jnp.int32(0)
    for j in range(n):
        total = total + jnp.where(dest_order[j] == device, j, 0)
    return total


def pack_kernel(counts, dest_order, *refs, n, per_peer, block_len, begin, width, with_ids):
    if with_ids:
        segments, hidden, out, sems, near, near_sem = refs
        fetch = pltpu.make_async_copy(segments, near, near_sem)
        fetch.start()
    else:
        hidden, out, sems = refs
    in_slots = hidden.shape[0] // block_len
    me = lax.axis_index("dp")
    mine = start_of(counts, me, n)
    slots = []
    copies = []
    for peer in range(n):
        offset = lax.rem(place_of(dest_order, peer, n) - mine + n * in_slots, n)
        for a in range(per_peer):
            slot = jnp.minimum(offset + a * n, in_slots - 1)
            row = pl.multiple_of(slot * block_len, block_len)
            copies.append(
                pltpu.make_async_copy(
                    hidden.at[pl.ds(row, block_len), pl.ds(begin, width)],
                    out.at[peer, a, pl.ds(0, block_len), :],
                    sems.at[peer, a],
                )
            )
            copies[-1].start()
            slots.append((peer, a, slot))
    if with_ids:
        fetch.wait()
        for peer, a, slot in slots:
            ids = near[pl.ds(slot, 1), :].astype(jnp.float32)
            ids = jnp.broadcast_to(ids, (ID_ROWS, block_len)).astype(jnp.bfloat16)
            out[peer, a, block_len:, :block_len] = ids
    for copy in copies:
        copy.wait()


def place_kernel(counts, dest_order, arrived, *outs, n, block_len, groups, with_ids):
    me = lax.axis_index("dp")
    my_place = place_of(dest_order, me, n)
    k = 0
    for g, size in enumerate(groups):
        for i in range(size):
            wanted = k * n + my_place
            source = jnp.int32(0)
            begin = jnp.int32(0)
            total = jnp.int32(0)
            for j in range(n):
                total = total + counts[j]
                passed = total <= wanted
                source = source + passed.astype(jnp.int32)
                begin = jnp.where(passed, total, begin)
            a = lax.div(wanted - begin, n)
            outs[g][i * block_len : (i + 1) * block_len, :] = arrived[source, a, :block_len, :]
            if with_ids:
                outs[-1][k] = arrived[source, a, block_len:, :block_len]
            k += 1


def fetch_kernel(q_weight, kv_weight, q_near, kv_near, q_sem, kv_sem):
    q_copy = pltpu.make_async_copy(q_weight, q_near, q_sem)
    kv_copy = pltpu.make_async_copy(kv_weight, kv_near, kv_sem)
    q_copy.start()
    kv_copy.start()
    q_copy.wait()
    kv_copy.wait()


def table_kernel(ids, cosines, sines, turn, cross, mask, *, kept, length):
    row = lax.broadcasted_iota(jnp.int32, (length, length), 0)
    column = lax.broadcasted_iota(jnp.int32, (length, length), 1)
    for k in range(kept):
        here = slice(k * length, (k + 1) * length)
        along = jnp.broadcast_to(ids[k, :1, :].astype(jnp.float32), (length, length))
        same = along == along.T
        visible = same & (column <= row)
        mask[here, :] = visible.astype(jnp.float32)
        before = (same & (column < row)).astype(jnp.float32)
        position = jnp.sum(before, axis=1, keepdims=True).astype(jnp.int32)
        chosen = (position == column).astype(jnp.float32)
        exact = dict(precision=lax.Precision.HIGHEST, preferred_element_type=jnp.float32)
        turn[here, :] = jnp.dot(chosen, cosines[...], **exact)
        cross[here, :] = jnp.dot(chosen, sines[...], **exact)


def relatives(me):
    inner = (me == 1) | (me == 2)
    pair = lax.bitwise_xor(me, 1)
    second = jnp.where(inner, 3 - me, jnp.where(me == 0, 2, 1))
    third = jnp.where(inner, lax.bitwise_xor(3 - me, 1), 3 - me)
    return inner, pair, second, third


def project_kernel(*refs, widths, first_rows):
    count = len(widths)
    pieces = refs[: 6 * count - 2]
    gain, q_weight, kv_weight, y, squares, x = refs[6 * count - 2 :]
    rows = x.shape[0]
    me = lax.axis_index("mp")
    inner, pair, second, third = relatives(me)
    local = sum(widths)
    begin = 0
    for c, width in enumerate(widths):
        row = slice(None) if first_rows[c] is None else slice(first_rows[c], first_rows[c] + rows)

        def put(source, value):
            column = pl.multiple_of(source * local + begin, HD)
            x[:, pl.ds(column, width)] = value

        if c < count - 1:
            own, near, mid, end_mid, far, end_far = pieces[6 * c : 6 * c + 6]
        else:
            own, near, mid, end_mid = pieces[6 * c :]
        put(me, own[row, :])
        put(pair, near[row, :])

        @pl.when(inner)
        def _():
            put(second, mid[row, :])

        @pl.when(jnp.logical_not(inner))
        def _():
            put(second, end_mid[row, :])

        if c < count - 1:

            @pl.when(inner)
            def _():
                put(third, far[row, :])

            @pl.when(jnp.logical_not(inner))
            def _():
                put(third, end_far[row, :])
        else:
            put(third, jnp.zeros((rows, width), x.dtype))

        begin += width
    total = jnp.zeros((rows, HD), jnp.float32)
    for t in range(x.shape[1] // HD):
        part = slice(t * HD, (t + 1) * HD)
        raw = x[:, part]
        wide = raw.astype(jnp.float32)
        total = total + wide * wide
        x[:, part] = raw * gain[:, part]
    squares[...] = total
    normed = x[...]
    split = q_weight.shape[1]
    y[:, :split] = jnp.dot(normed, q_weight[...], preferred_element_type=jnp.float32)
    y[:, split:] = jnp.dot(normed, kv_weight[...], preferred_element_type=jnp.float32)


def attend_kernel(*refs, first, low, q_heads, kv_local, fresh):
    far, end_far, y_part, squares, gain, turn, cross, mask, q_weight, kv_weight = refs[:10]
    out, x, y, stage, out_sem = refs[10 if fresh else 11 :]
    rows, width = x.shape
    me = lax.axis_index("mp")
    inner, _, _, third = relatives(me)
    depth = q_weight.shape[0]

    @pl.when(inner)
    def _():
        x[...] = far[...]

    @pl.when(jnp.logical_not(inner))
    def _():
        x[...] = end_far[...]

    total = squares[...]
    for t in range(width // HD):
        wide = x[:, t * HD : (t + 1) * HD].astype(jnp.float32)
        total = total + wide * wide
    scale = lax.rsqrt(jnp.sum(total, axis=1, keepdims=True) / depth + epsilon)
    part = pl.ds(pl.multiple_of(third * (depth // 4) + first, HD), width)
    normed = x[...] * gain[:, part]
    split = q_heads * HD
    y[:, :split] = y_part[:, :split] + jnp.dot(
        normed, q_weight[part, :], preferred_element_type=jnp.float32
    )
    y[:, split:] = y_part[:, split:] + jnp.dot(
        normed, kv_weight[part, :], preferred_element_type=jnp.float32
    )
    per_kv = q_heads // kv_local
    length = mask.shape[1]
    for b in range(rows // length):
        here = slice(b * length, (b + 1) * length)
        row_scale = scale[here]
        there = slice(low + b * length, low + (b + 1) * length)
        cosine = turn[there, :]
        sine = cross[there, :]
        visible = mask[there, :] > 0

        def rotated(value):
            return (value * cosine + pltpu.roll(value, HD // 2, 1) * sine).astype(jnp.bfloat16)

        visible_all = jnp.concatenate([visible] * per_kv, axis=0)
        for j in range(kv_local):
            base = q_heads * HD + 2 * j * HD
            key = (row_scale * y[here, base : base + HD]).astype(jnp.bfloat16)
            key = rotated(key.astype(jnp.float32))
            value = (row_scale * y[here, base + HD : base + 2 * HD]).astype(jnp.bfloat16)
            query = jnp.concatenate(
                [
                    rotated(row_scale * y[here, h * HD : (h + 1) * HD])
                    for h in range(j * per_kv, (j + 1) * per_kv)
                ],
                axis=0,
            )
            scores = lax.dot_general(
                query, key, (((1,), (1,)), ((), ())), preferred_element_type=jnp.float32
            ) * HD ** (-0.5)
            scores = jnp.where(visible_all, scores, -jnp.inf)
            highest = jnp.max(scores, axis=1, keepdims=True)
            weights = jnp.exp(scores - highest)
            shares = (weights / jnp.sum(weights, axis=1, keepdims=True)).astype(jnp.bfloat16)
            mixed = jnp.dot(shares, value, preferred_element_type=jnp.float32).astype(jnp.bfloat16)
            for i in range(per_kv):
                h = j * per_kv + i
                stage[here, h * HD : (h + 1) * HD] = mixed[i * length : (i + 1) * length]
    copy = pltpu.make_async_copy(stage, out.at[pl.ds(low, rows), :], out_sem)
    copy.start()
    copy.wait()


PAIRS = [(0, 1), (1, 0), (2, 3), (3, 2)]
MIDDLE = [(1, 2), (2, 1)]
OUTWARD = [(1, 0), (2, 3)]


def send(value, pairs):
    return lax.ppermute(value, "mp", pairs)


def table_values(length):
    frequency = np.float32(rope_base) ** (-(np.arange(HD // 2, dtype=np.float32) * 2) / HD)
    angles = np.arange(length, dtype=np.float32)[:, None] * frequency.astype(np.float32)
    cosine, sine = np.cos(angles), np.sin(angles)
    both = (np.concatenate([cosine, cosine], 1), np.concatenate([-sine, sine], 1))
    return tuple(jnp.asarray(v, jnp.float32) for v in both)


def line_device(hidden, segments, counts, dest_order, norm_gain, q_weight, kv_weight):
    n = lax.axis_size("dp")
    in_slots, block_len = segments.shape
    kept = in_slots // 2
    per_peer = (in_slots + n - 1) // n
    local = hidden.shape[1]
    tokens = kept * block_len
    q_heads = q_weight.shape[1] // HD
    kv_local = kv_weight.shape[1] // (2 * HD)
    bf16 = jnp.bfloat16
    widths = tuple(local * e // 8 for e in FEATURE_EIGHTHS)
    dma = pltpu.SemaphoreType.DMA
    packed = []
    for c, width in enumerate(widths):
        height = block_len + (ID_ROWS if c == 0 else 0)
        scratch = [dma((n, per_peer))]
        if c == 0:
            scratch += [pltpu.VMEM(segments.shape, jnp.int32), dma(())]
        operands = ([segments] if c == 0 else []) + [hidden]
        packed.append(
            pl.pallas_call(
                functools.partial(
                    pack_kernel,
                    n=n,
                    per_peer=per_peer,
                    block_len=block_len,
                    begin=sum(widths[:c]),
                    width=width,
                    with_ids=c == 0,
                ),
                out_shape=pltpu.VMEM((n, per_peer, height, width), bf16),
                in_specs=[SMEM, SMEM] + [ANY] * len(operands),
                out_specs=VMEM,
                scratch_shapes=scratch,
                compiler_params=limit(8),
            )(*[afar(operand) for operand in [counts, dest_order] + operands])
        )
    q_near, kv_near = pl.pallas_call(
        fetch_kernel,
        out_shape=[pltpu.VMEM(w.shape, bf16) for w in (q_weight, kv_weight)],
        in_specs=[ANY, ANY],
        out_specs=[VMEM, VMEM],
        scratch_shapes=[dma(()), dma(())],
        compiler_params=limit(4),
        name="fetch",
    )(afar(q_weight), afar(kv_weight))
    came = []
    for buffer in packed:
        came.append(lax.all_to_all(buffer, "dp", split_axis=0, concat_axis=0, tiled=True))
    gathered = []
    block_ids = None
    for c, (width, arrived) in enumerate(zip(widths, came)):
        groups = GROUPS if c == len(widths) - 1 else (kept,)
        shapes = [pltpu.VMEM((size * block_len, width), bf16) for size in groups]
        if c == 0:
            shapes.append(pltpu.VMEM((kept, ID_ROWS, block_len), bf16))
        placed = pl.pallas_call(
            functools.partial(
                place_kernel, n=n, block_len=block_len, groups=groups, with_ids=c == 0
            ),
            out_shape=shapes,
            in_specs=[SMEM, SMEM, VMEM],
            out_specs=[VMEM] * len(shapes),
            compiler_params=limit(4),
        )(afar(counts), afar(dest_order), resident(arrived))
        if c == 0:
            block_ids = placed[-1]
            placed = placed[:-1]
        rows = []
        for own in placed:
            near = send(own, PAIRS)
            mid = send(own, MIDDLE)
            far = send(near, MIDDLE)
            end_mid = send(mid, OUTWARD)
            end_far = send(far, OUTWARD)
            rows.append([own, near, mid, far, end_mid, end_far])
        gathered.append(rows)
    cosine, sine = table_values(block_len)
    turn, cross, mask = pl.pallas_call(
        functools.partial(table_kernel, kept=kept, length=block_len),
        out_shape=[pltpu.VMEM((tokens, HD), jnp.float32)] * 2
        + [pltpu.VMEM((tokens, block_len), jnp.float32)],
        in_specs=[VMEM] * 3,
        out_specs=[VMEM] * 3,
        compiler_params=limit(4),
        name="tables",
    )(resident(block_ids), resident(cosine), resident(sine))
    gain = norm_gain[None, :]
    columns = q_weight.shape[1] + kv_weight.shape[1]
    last = len(widths) - 1
    out = None
    low = 0
    for g, size in enumerate(GROUPS):
        rows = size * block_len
        pieces, first_rows = [], []
        for c in range(len(widths)):
            whole = c < last
            own, near, mid, far, end_mid, end_far = gathered[c][0 if whole else g]
            pieces += [own, near, mid, end_mid] + ([far, end_far] if whole else [])
            first_rows.append(low if whole else None)
        operands = pieces + [gain, q_near, kv_near]
        flops = 2 * rows * q_weight.shape[0] * columns
        y, squares = pl.pallas_call(
            functools.partial(project_kernel, widths=widths, first_rows=tuple(first_rows)),
            out_shape=[
                pltpu.VMEM((rows, columns), jnp.float32),
                pltpu.VMEM((rows, HD), jnp.float32),
            ],
            in_specs=[VMEM] * len(operands),
            out_specs=[VMEM] * 2,
            scratch_shapes=[pltpu.VMEM((rows, 4 * local), bf16)],
            compiler_params=limit(12),
            cost_estimate=pl.CostEstimate(flops=flops, transcendentals=0, bytes_accessed=16 * MIB),
        )(*[resident(operand) for operand in operands])
        operands = [far, end_far, y, squares, gain, turn, cross, mask, q_near, kv_near]
        operands = [resident(operand) for operand in operands]
        specs = [VMEM] * len(operands)
        aliases = {}
        if out is not None:
            aliases = {len(operands): 0}
            operands.append(out)
            specs.append(ANY)
        out = pl.pallas_call(
            functools.partial(
                attend_kernel,
                first=sum(widths[:last]),
                low=low,
                q_heads=q_heads,
                kv_local=kv_local,
                fresh=out is None,
            ),
            out_shape=jax.ShapeDtypeStruct((tokens, q_heads * HD), bf16),
            in_specs=specs,
            out_specs=ANY,
            input_output_aliases=aliases,
            scratch_shapes=[
                pltpu.VMEM((rows, widths[last]), bf16),
                pltpu.VMEM((rows, columns), jnp.float32),
                pltpu.VMEM((rows, q_heads * HD), bf16),
                dma(()),
            ],
            compiler_params=limit(12),
            cost_estimate=pl.CostEstimate(
                flops=flops // 4, transcendentals=0, bytes_accessed=4 * MIB
            ),
        )(*operands)
        low += rows
    return out


def solution(mesh):
    in_specs = (P("dp", "mp"), P("dp", None), P(), P(), P(), P(None, "mp"), P(None, "mp"))
    out_specs = P("dp", "mp")
    mp_count = mesh.shape["mp"]
    line = mp_count == 4 and KV % mp_count == 0

    def body(*arrays):
        return line_device(*arrays)

    return jax.shard_map(
        body if line else general_device,
        mesh=mesh,
        in_specs=in_specs,
        out_specs=out_specs,
        check_vma=False,
    )
```

```python
import functools

import jax
import jax.numpy as jnp
import numpy as np
from jax import lax
from jax.experimental import pallas as pl
from jax.experimental.pallas import tpu as pltpu
from jax.sharding import PartitionSpec as P

KV = 8
HD = 128


epsilon = 1e-05
rope_base = 500000.0

ID_ROWS = 8
FEATURE_EIGHTHS = (1, 2, 5)
GROUPS = (3, 3, 2)


def for_sending(array):
    return jax.tree.map(lambda a: a.astype(jnp.bfloat16) if a.dtype == jnp.float32 else a, array)


def swapped(value, axis, stride):
    mask = 2**stride
    pairs = [(source, source ^ mask) for source in range(lax.axis_size(axis))]
    return lax.ppermute(value, axis, pairs)


def rope_tables(positions, width):
    halves = width // 2
    frequency = rope_base ** (-(jnp.arange(halves, dtype=jnp.float32) * 2.0) / width)
    angles = positions.astype(jnp.float32)[..., None] * frequency
    return (jnp.cos(angles), jnp.sin(angles))


def rotate(tensor, cosine, sine_part):
    halves = tensor.shape[-1] // 2
    lower = tensor[..., :halves]
    upper = tensor[..., halves:]
    cosine = cosine[..., None, :]
    sine_part = sine_part[..., None, :]
    return jnp.concatenate(
        [lower * cosine - upper * sine_part, upper * cosine + lower * sine_part], axis=-1
    )


def segment_masks(block_segments):
    length = block_segments.shape[-1]
    column = jnp.arange(length, dtype=jnp.int32)
    same_segment = block_segments[:, :, None] == block_segments[:, None, :]
    before = column[None, :] < column[:, None]
    positions = jnp.sum((same_segment & before[None]).astype(jnp.int32), axis=2)
    visible = same_segment & (column[None, :] <= column[:, None])[None]
    return (positions, visible)


def join_pieces(mine, theirs, upper_half):
    halves = mine.shape[-1] // 2
    leading = jnp.where(upper_half, theirs, mine)
    trailing = jnp.where(upper_half, mine, theirs)
    return jnp.concatenate(
        [leading[:, :halves], trailing[:, :halves], leading[:, halves:], trailing[:, halves:]],
        axis=-1,
    )


def general_device(hidden, segments, counts, dest_order, norm_gain, q_weight, kv_weight):
    dp_count = lax.axis_size("dp")
    mp_count = lax.axis_size("mp")
    dp_index = lax.axis_index("dp")
    mp_index = lax.axis_index("mp")
    in_slots = segments.shape[0]
    block_len = segments.shape[1]
    kept_slots = in_slots // 2
    per_peer = (in_slots + dp_count - 1) // dp_count
    local_width = hidden.shape[1]
    head_share = max(1, mp_count // KV)
    kv_local = max(1, KV // mp_count)
    token_count = kept_slots * block_len
    device_ids = jnp.arange(dp_count, dtype=jnp.int32)
    starts = jnp.cumsum(counts) - counts
    finishes = starts + counts
    position_of = jnp.sum(
        device_ids[None, :] * (dest_order[None, :] == device_ids[:, None]).astype(jnp.int32), axis=1
    )
    offsets = (position_of - starts[dp_index]) % dp_count
    wanted = offsets[:, None] + jnp.arange(per_peer, dtype=jnp.int32)[None, :] * dp_count
    usable = wanted < counts[dp_index]
    slot_ids = jnp.arange(in_slots, dtype=jnp.int32)
    choose = ((wanted[:, :, None] == slot_ids[None, None, :]) & usable[:, :, None]).astype(
        jnp.bfloat16
    )
    choose = choose.reshape(dp_count * per_peer, in_slots)
    outgoing = jnp.dot(
        choose,
        hidden.reshape(in_slots, block_len * local_width),
        preferred_element_type=jnp.float32,
    ).astype(jnp.bfloat16)
    segment_out = jnp.dot(
        choose, segments.astype(jnp.bfloat16), preferred_element_type=jnp.float32
    ).astype(jnp.bfloat16)
    global_ids = jnp.arange(kept_slots, dtype=jnp.int32) * dp_count + position_of[dp_index]
    sources = jnp.sum((finishes[None, :] <= global_ids[:, None]).astype(jnp.int32), axis=1)
    arrive_rows = sources * per_peer + (global_ids - starts[sources]) // dp_count
    place = (
        arrive_rows[:, None] == jnp.arange(dp_count * per_peer, dtype=jnp.int32)[None, :]
    ).astype(jnp.bfloat16)
    arrived = lax.all_to_all(
        outgoing.reshape(dp_count, per_peer, block_len * local_width),
        "dp",
        split_axis=0,
        concat_axis=0,
        tiled=True,
    )
    segment_in = lax.all_to_all(
        segment_out.reshape(dp_count, per_peer, block_len),
        "dp",
        split_axis=0,
        concat_axis=0,
        tiled=True,
    )
    block_rows = arrived.astype(jnp.float32).reshape(dp_count, per_peer, block_len, local_width)
    arrived_squares = jnp.sum(block_rows * block_rows, axis=3)
    placed_squares = jnp.dot(
        place.astype(jnp.float32),
        arrived_squares.reshape(dp_count * per_peer, block_len),
        precision=lax.Precision.HIGHEST,
    ).reshape(token_count)
    rows = jnp.dot(
        place,
        arrived.reshape(dp_count * per_peer, block_len * local_width),
        preferred_element_type=jnp.float32,
    ).astype(jnp.bfloat16)
    rows = rows.reshape(token_count, local_width)
    block_segments = jnp.dot(
        place,
        segment_in.reshape(dp_count * per_peer, block_len),
        preferred_element_type=jnp.float32,
    )
    widened = rows.astype(jnp.float32)
    totals = lax.psum(placed_squares, "mp")
    row_scale = lax.rsqrt(totals / norm_gain.shape[0] + epsilon)[:, None]
    local_gain = lax.dynamic_slice_in_dim(norm_gain, mp_index * local_width, local_width)
    gained = (widened * local_gain.astype(jnp.float32)).astype(jnp.bfloat16)
    normed = lax.all_gather(gained, "mp", axis=1, tiled=True)
    queries = row_scale * jnp.dot(normed, q_weight, preferred_element_type=jnp.float32)
    kv_rows = (row_scale * jnp.dot(normed, kv_weight, preferred_element_type=jnp.float32)).astype(
        jnp.bfloat16
    )
    for level in range(head_share.bit_length() - 1):
        theirs = swapped(for_sending(kv_rows), "mp", level).astype(kv_rows.dtype)
        upper_half = mp_index // (1 << level) % 2 == 1
        kv_rows = join_pieces(kv_rows, theirs, upper_half)
    kv_split = kv_rows.reshape(token_count, kv_local, 2, HD)
    key_raw = kv_split[:, :, 0, :]
    value_rows = kv_split[:, :, 1, :]
    positions, visible = segment_masks(block_segments)
    cosine, sine_part = rope_tables(positions, HD)
    q_heads = queries.shape[1] // HD
    query_rows = rotate(
        queries.reshape(kept_slots, block_len, q_heads, HD), cosine, sine_part
    ).astype(jnp.bfloat16)
    key_rows = rotate(
        key_raw.astype(jnp.float32).reshape(kept_slots, block_len, kv_local, HD), cosine, sine_part
    ).astype(jnp.bfloat16)
    grouped = query_rows.reshape(kept_slots, block_len, kv_local, q_heads // kv_local, HD)
    scores = jnp.einsum(
        "nikgd,njkd->nkgij", grouped, key_rows, preferred_element_type=jnp.float32
    ) * HD ** (-0.5)
    scores = jnp.where(visible[:, None, None], scores, -jnp.inf)
    highest = jnp.max(scores, axis=-1, keepdims=True)
    weights = jnp.exp(scores - highest)
    shares = (weights / jnp.sum(weights, axis=-1, keepdims=True)).astype(jnp.bfloat16)
    values = value_rows.reshape(kept_slots, block_len, kv_local, HD)
    mixture = jnp.einsum("nkgij,njkd->nikgd", shares, values, preferred_element_type=jnp.float32)
    return mixture.reshape(token_count, q_heads * HD).astype(jnp.bfloat16)


ANY = pl.BlockSpec(memory_space=pl.ANY)
SMEM = pl.BlockSpec(memory_space=pltpu.SMEM)
VMEM = pl.BlockSpec(memory_space=pltpu.VMEM)
MIB = 1024 * 1024


def resident(value):
    return pltpu.with_memory_space_constraint(value, pltpu.VMEM)


def afar(value):
    return pltpu.with_memory_space_constraint(value, pltpu.HBM)


def limit(mib):
    return pltpu.CompilerParams(vmem_limit_bytes=mib * MIB)


def start_of(counts, index, n):
    total = jnp.int32(0)
    for j in range(n):
        total = total + jnp.where(j < index, counts[j], 0)
    return total


def place_of(dest_order, device, n):
    total = jnp.int32(0)
    for j in range(n):
        total = total + jnp.where(dest_order[j] == device, j, 0)
    return total


def pack_kernel(counts, dest_order, *refs, n, per_peer, block_len, begin, width, with_ids):
    if with_ids:
        segments, hidden, out, sems, near, near_sem = refs
        fetch = pltpu.make_async_copy(segments, near, near_sem)
        fetch.start()
    else:
        hidden, outs, sems = refs[0], refs[1 : n + 1], refs[n + 1]
    in_slots = hidden.shape[0] // block_len
    me = lax.axis_index("dp")
    mine = start_of(counts, me, n)
    slots = []
    copies = []
    for r in range(n):
        peer = r if with_ids else lax.bitwise_xor(me, r)
        offset = lax.rem(place_of(dest_order, peer, n) - mine + n * in_slots, n)
        for a in range(per_peer):
            slot = jnp.minimum(offset + a * n, in_slots - 1)
            row = pl.multiple_of(slot * block_len, block_len)
            target = out.at[r, a, pl.ds(0, block_len), :] if with_ids else outs[r].at[a]
            copies.append(
                pltpu.make_async_copy(
                    hidden.at[pl.ds(row, block_len), pl.ds(begin, width)], target, sems.at[r, a]
                )
            )
            copies[-1].start()
            slots.append((r, a, slot))
    if with_ids:
        fetch.wait()
        for r, a, slot in slots:
            ids = near[pl.ds(slot, 1), :].astype(jnp.float32)
            ids = jnp.broadcast_to(ids, (ID_ROWS, block_len)).astype(jnp.bfloat16)
            out[r, a, block_len:, :block_len] = ids
    for copy in copies:
        copy.wait()


def place_kernel(counts, dest_order, *refs, n, block_len, groups, with_ids):
    count = 1 if with_ids else n
    arrived, outs = refs[:count], refs[count:]
    me = lax.axis_index("dp")
    my_place = place_of(dest_order, me, n)
    k = 0
    for g, size in enumerate(groups):
        for i in range(size):
            wanted = k * n + my_place
            source = jnp.int32(0)
            begin = jnp.int32(0)
            total = jnp.int32(0)
            for j in range(n):
                total = total + counts[j]
                passed = total <= wanted
                source = source + passed.astype(jnp.int32)
                begin = jnp.where(passed, total, begin)
            a = lax.div(wanted - begin, n)
            here = slice(i * block_len, (i + 1) * block_len)
            if with_ids:
                outs[g][here, :] = arrived[0][source, a, :block_len, :]
                outs[-1][k] = arrived[0][source, a, block_len:, :block_len]
            else:
                came_by = lax.bitwise_xor(source, me)
                for r in range(n):

                    @pl.when(came_by == r)
                    def _():
                        outs[g][here, :] = arrived[r][a]

            k += 1


def fetch_kernel(q_weight, kv_weight, q_near, kv_near, q_sem, kv_sem):
    q_copy = pltpu.make_async_copy(q_weight, q_near, q_sem)
    kv_copy = pltpu.make_async_copy(kv_weight, kv_near, kv_sem)
    q_copy.start()
    kv_copy.start()
    q_copy.wait()
    kv_copy.wait()


def table_kernel(ids, cosines, sines, turn, cross, mask, *, kept, length):
    row = lax.broadcasted_iota(jnp.int32, (length, length), 0)
    column = lax.broadcasted_iota(jnp.int32, (length, length), 1)
    for k in range(kept):
        here = slice(k * length, (k + 1) * length)
        along = jnp.broadcast_to(ids[k, :1, :].astype(jnp.float32), (length, length))
        same = along == along.T
        visible = same & (column <= row)
        mask[here, :] = visible.astype(jnp.float32)
        before = (same & (column < row)).astype(jnp.float32)
        position = jnp.sum(before, axis=1, keepdims=True).astype(jnp.int32)
        chosen = (position == column).astype(jnp.float32)
        exact = dict(precision=lax.Precision.HIGHEST, preferred_element_type=jnp.float32)
        turn[here, :] = jnp.dot(chosen, cosines[...], **exact)
        cross[here, :] = jnp.dot(chosen, sines[...], **exact)


def relatives(me):
    inner = (me == 1) | (me == 2)
    pair = lax.bitwise_xor(me, 1)
    second = jnp.where(inner, 3 - me, jnp.where(me == 0, 2, 1))
    third = jnp.where(inner, lax.bitwise_xor(3 - me, 1), 3 - me)
    return inner, pair, second, third


def project_kernel(*refs, widths, first_rows):
    count = len(widths)
    pieces = refs[: 6 * count - 2]
    gain, q_weight, kv_weight, y, squares, x = refs[6 * count - 2 :]
    rows = x.shape[0]
    me = lax.axis_index("mp")
    inner, pair, second, third = relatives(me)
    local = sum(widths)
    begin = 0
    for c, width in enumerate(widths):
        row = slice(None) if first_rows[c] is None else slice(first_rows[c], first_rows[c] + rows)

        def put(source, value):
            column = pl.multiple_of(source * local + begin, HD)
            x[:, pl.ds(column, width)] = value

        if c < count - 1:
            own, near, mid, end_mid, far, end_far = pieces[6 * c : 6 * c + 6]
        else:
            own, near, mid, end_mid = pieces[6 * c :]
        put(me, own[row, :])
        put(pair, near[row, :])

        @pl.when(inner)
        def _():
            put(second, mid[row, :])

        @pl.when(jnp.logical_not(inner))
        def _():
            put(second, end_mid[row, :])

        if c < count - 1:

            @pl.when(inner)
            def _():
                put(third, far[row, :])

            @pl.when(jnp.logical_not(inner))
            def _():
                put(third, end_far[row, :])
        else:
            put(third, jnp.zeros((rows, width), x.dtype))

        begin += width
    total = jnp.zeros((rows, HD), jnp.float32)
    for t in range(x.shape[1] // HD):
        part = slice(t * HD, (t + 1) * HD)
        raw = x[:, part]
        wide = raw.astype(jnp.float32)
        total = total + wide * wide
        x[:, part] = raw * gain[:, part]
    squares[...] = total
    normed = x[...]
    split = q_weight.shape[1]
    y[:, :split] = jnp.dot(normed, q_weight[...], preferred_element_type=jnp.float32)
    y[:, split:] = jnp.dot(normed, kv_weight[...], preferred_element_type=jnp.float32)


def attend_kernel(*refs, first, low, q_heads, kv_local, fresh):
    far, end_far, y_part, squares, gain, turn, cross, mask, q_weight, kv_weight = refs[:10]
    out, x, y, stage, out_sem = refs[10 if fresh else 11 :]
    rows, width = x.shape
    me = lax.axis_index("mp")
    inner, _, _, third = relatives(me)
    depth = q_weight.shape[0]

    @pl.when(inner)
    def _():
        x[...] = far[...]

    @pl.when(jnp.logical_not(inner))
    def _():
        x[...] = end_far[...]

    total = squares[...]
    for t in range(width // HD):
        wide = x[:, t * HD : (t + 1) * HD].astype(jnp.float32)
        total = total + wide * wide
    scale = lax.rsqrt(jnp.sum(total, axis=1, keepdims=True) / depth + epsilon)
    part = pl.ds(pl.multiple_of(third * (depth // 4) + first, HD), width)
    normed = x[...] * gain[:, part]
    split = q_heads * HD
    y[:, :split] = y_part[:, :split] + jnp.dot(
        normed, q_weight[part, :], preferred_element_type=jnp.float32
    )
    y[:, split:] = y_part[:, split:] + jnp.dot(
        normed, kv_weight[part, :], preferred_element_type=jnp.float32
    )
    per_kv = q_heads // kv_local
    length = mask.shape[1]
    for b in range(rows // length):
        here = slice(b * length, (b + 1) * length)
        row_scale = scale[here]
        there = slice(low + b * length, low + (b + 1) * length)
        cosine = turn[there, :]
        sine = cross[there, :]
        visible = mask[there, :] > 0

        def rotated(value):
            return (value * cosine + pltpu.roll(value, HD // 2, 1) * sine).astype(jnp.bfloat16)

        visible_all = jnp.concatenate([visible] * per_kv, axis=0)
        for j in range(kv_local):
            base = q_heads * HD + 2 * j * HD
            key = (row_scale * y[here, base : base + HD]).astype(jnp.bfloat16)
            key = rotated(key.astype(jnp.float32))
            value = (row_scale * y[here, base + HD : base + 2 * HD]).astype(jnp.bfloat16)
            query = jnp.concatenate(
                [
                    rotated(row_scale * y[here, h * HD : (h + 1) * HD])
                    for h in range(j * per_kv, (j + 1) * per_kv)
                ],
                axis=0,
            )
            scores = lax.dot_general(
                query, key, (((1,), (1,)), ((), ())), preferred_element_type=jnp.float32
            ) * HD ** (-0.5)
            scores = jnp.where(visible_all, scores, -jnp.inf)
            highest = jnp.max(scores, axis=1, keepdims=True)
            weights = jnp.exp(scores - highest)
            shares = (weights / jnp.sum(weights, axis=1, keepdims=True)).astype(jnp.bfloat16)
            mixed = jnp.dot(shares, value, preferred_element_type=jnp.float32).astype(jnp.bfloat16)
            for i in range(per_kv):
                h = j * per_kv + i
                stage[here, h * HD : (h + 1) * HD] = mixed[i * length : (i + 1) * length]
    copy = pltpu.make_async_copy(stage, out.at[pl.ds(low, rows), :], out_sem)
    copy.start()
    copy.wait()


PAIRS = [(0, 1), (1, 0), (2, 3), (3, 2)]
MIDDLE = [(1, 2), (2, 1)]
OUTWARD = [(1, 0), (2, 3)]


def send(value, pairs):
    return lax.ppermute(value, "mp", pairs)


def table_values(length):
    frequency = np.float32(rope_base) ** (-(np.arange(HD // 2, dtype=np.float32) * 2) / HD)
    angles = np.arange(length, dtype=np.float32)[:, None] * frequency.astype(np.float32)
    cosine, sine = np.cos(angles), np.sin(angles)
    both = (np.concatenate([cosine, cosine], 1), np.concatenate([-sine, sine], 1))
    return tuple(jnp.asarray(v, jnp.float32) for v in both)


def line_device(hidden, segments, counts, dest_order, norm_gain, q_weight, kv_weight):
    n = lax.axis_size("dp")
    in_slots, block_len = segments.shape
    kept = in_slots // 2
    per_peer = (in_slots + n - 1) // n
    local = hidden.shape[1]
    tokens = kept * block_len
    q_heads = q_weight.shape[1] // HD
    kv_local = kv_weight.shape[1] // (2 * HD)
    bf16 = jnp.bfloat16
    widths = tuple(local * e // 8 for e in FEATURE_EIGHTHS)
    dma = pltpu.SemaphoreType.DMA
    packed = []
    for c, width in enumerate(widths):
        height = block_len + (ID_ROWS if c == 0 else 0)
        scratch = [dma((n, per_peer))]
        if c == 0:
            scratch += [pltpu.VMEM(segments.shape, jnp.int32), dma(())]
        operands = ([segments] if c == 0 else []) + [hidden]
        packed.append(
            pl.pallas_call(
                functools.partial(
                    pack_kernel,
                    n=n,
                    per_peer=per_peer,
                    block_len=block_len,
                    begin=sum(widths[:c]),
                    width=width,
                    with_ids=c == 0,
                ),
                out_shape=pltpu.VMEM((n, per_peer, height, width), bf16)
                if c == 0
                else [pltpu.VMEM((per_peer, height, width), bf16)] * n,
                in_specs=[SMEM, SMEM] + [ANY] * len(operands),
                out_specs=VMEM if c == 0 else [VMEM] * n,
                scratch_shapes=scratch,
                compiler_params=limit(8),
            )(*[afar(operand) for operand in [counts, dest_order] + operands])
        )
    q_near, kv_near = pl.pallas_call(
        fetch_kernel,
        out_shape=[pltpu.VMEM(w.shape, bf16) for w in (q_weight, kv_weight)],
        in_specs=[ANY, ANY],
        out_specs=[VMEM, VMEM],
        scratch_shapes=[dma(()), dma(())],
        compiler_params=limit(4),
        name="fetch",
    )(afar(q_weight), afar(kv_weight))
    came = []
    for c, buffers in enumerate(packed):
        if c == 0:
            came.append([lax.all_to_all(buffers, "dp", split_axis=0, concat_axis=0, tiled=True)])
            continue
        came.append([buffers[0]])
        for r in range(1, n):
            pairs = [(i, i ^ r) for i in range(n)]
            came[-1].append(lax.ppermute(buffers[r], "dp", pairs))
    gathered = []
    block_ids = None
    for c, (width, arrived) in enumerate(zip(widths, came)):
        groups = GROUPS if c == len(widths) - 1 else (kept,)
        shapes = [pltpu.VMEM((size * block_len, width), bf16) for size in groups]
        if c == 0:
            shapes.append(pltpu.VMEM((kept, ID_ROWS, block_len), bf16))
        placed = pl.pallas_call(
            functools.partial(
                place_kernel, n=n, block_len=block_len, groups=groups, with_ids=c == 0
            ),
            out_shape=shapes,
            in_specs=[SMEM, SMEM] + [VMEM] * len(arrived),
            out_specs=[VMEM] * len(shapes),
            compiler_params=limit(4),
        )(afar(counts), afar(dest_order), *[resident(part) for part in arrived])
        if c == 0:
            block_ids = placed[-1]
            placed = placed[:-1]
        rows = []
        for own in placed:
            near = send(own, PAIRS)
            mid = send(own, MIDDLE)
            far = send(near, MIDDLE)
            end_mid = send(mid, OUTWARD)
            end_far = send(far, OUTWARD)
            rows.append([own, near, mid, far, end_mid, end_far])
        gathered.append(rows)
    cosine, sine = table_values(block_len)
    turn, cross, mask = pl.pallas_call(
        functools.partial(table_kernel, kept=kept, length=block_len),
        out_shape=[pltpu.VMEM((tokens, HD), jnp.float32)] * 2
        + [pltpu.VMEM((tokens, block_len), jnp.float32)],
        in_specs=[VMEM] * 3,
        out_specs=[VMEM] * 3,
        compiler_params=limit(4),
        name="tables",
    )(resident(block_ids), resident(cosine), resident(sine))
    gain = norm_gain[None, :]
    columns = q_weight.shape[1] + kv_weight.shape[1]
    last = len(widths) - 1
    out = None
    low = 0
    for g, size in enumerate(GROUPS):
        rows = size * block_len
        pieces, first_rows = [], []
        for c in range(len(widths)):
            whole = c < last
            own, near, mid, far, end_mid, end_far = gathered[c][0 if whole else g]
            pieces += [own, near, mid, end_mid] + ([far, end_far] if whole else [])
            first_rows.append(low if whole else None)
        operands = pieces + [gain, q_near, kv_near]
        flops = 2 * rows * q_weight.shape[0] * columns
        y, squares = pl.pallas_call(
            functools.partial(project_kernel, widths=widths, first_rows=tuple(first_rows)),
            out_shape=[
                pltpu.VMEM((rows, columns), jnp.float32),
                pltpu.VMEM((rows, HD), jnp.float32),
            ],
            in_specs=[VMEM] * len(operands),
            out_specs=[VMEM] * 2,
            scratch_shapes=[pltpu.VMEM((rows, 4 * local), bf16)],
            compiler_params=limit(12),
            cost_estimate=pl.CostEstimate(flops=flops, transcendentals=0, bytes_accessed=16 * MIB),
        )(*[resident(operand) for operand in operands])
        operands = [far, end_far, y, squares, gain, turn, cross, mask, q_near, kv_near]
        operands = [resident(operand) for operand in operands]
        specs = [VMEM] * len(operands)
        aliases = {}
        if out is not None:
            aliases = {len(operands): 0}
            operands.append(out)
            specs.append(ANY)
        out = pl.pallas_call(
            functools.partial(
                attend_kernel,
                first=sum(widths[:last]),
                low=low,
                q_heads=q_heads,
                kv_local=kv_local,
                fresh=out is None,
            ),
            out_shape=jax.ShapeDtypeStruct((tokens, q_heads * HD), bf16),
            in_specs=specs,
            out_specs=ANY,
            input_output_aliases=aliases,
            scratch_shapes=[
                pltpu.VMEM((rows, widths[last]), bf16),
                pltpu.VMEM((rows, columns), jnp.float32),
                pltpu.VMEM((rows, q_heads * HD), bf16),
                dma(()),
            ],
            compiler_params=limit(12),
            cost_estimate=pl.CostEstimate(
                flops=flops // 4, transcendentals=0, bytes_accessed=4 * MIB
            ),
        )(*operands)
        low += rows
    return out


def solution(mesh):
    in_specs = (P("dp", "mp"), P("dp", None), P(), P(), P(), P(None, "mp"), P(None, "mp"))
    out_specs = P("dp", "mp")
    dp_count, mp_count = mesh.shape["dp"], mesh.shape["mp"]
    line = mp_count == 4 and dp_count == 8 and KV % mp_count == 0

    def body(*arrays):
        return line_device(*arrays)

    return jax.shard_map(
        body if line else general_device,
        mesh=mesh,
        in_specs=in_specs,
        out_specs=out_specs,
        check_vma=False,
    )
```
